256 devices in a mesh: phase: 16 (over y, x), line: 16 (over z, core).
Axes of the slice: x: 4, y: 4, z: 8, core: 2. Of those that a mesh axis runs over, the one named last changes fastest.
Arguments:
- signal: bfloat16 [16, 16, 8192, 256], P('phase', 'line'), may hold values from -8 to 8, as said below
- tap_gain: float32 [3, 256], replicated, may hold values from 0.3 to 1.2
Outputs:
- echoed: bfloat16 [16, 16, 8192, 256], P('phase', 'line')
The draws below stay inside these ranges and needn't reach their ends.
Inputs may be any that keep to these rules, and one draw needn't show every extreme that they name: signal holds numbers from -8 to 8.
All inputs are finite; a program needn't handle non-finite values.
Results may differ from the reference program's by a relative error of at most 0.0055.
Values may be sent and summed in bfloat16 or wider, within the bound.
A program may use at most 64 MiB of HBM per device.

```python
import jax
import jax.numpy as jnp
from jax import lax

STEPS_DEV = 8192
CHANNELS = 256
SEGMENTS = 16
RECORDS = 16


def draw_signal(key, part):
    keys = jax.random.split(key, 2)
    loud = jnp.exp(jax.random.uniform(keys[0], (SEGMENTS, RECORDS, 1, CHANNELS), jnp.float32, -1.2, 1.2))
    noise = jax.random.normal(keys[1], (SEGMENTS, RECORDS, STEPS_DEV, CHANNELS), jnp.float32)
    return jnp.clip(loud * noise, -8.0, 8.0).astype(jnp.bfloat16)


def setup_inputs(seed: int = 0) -> dict:
    arg_keys = jax.random.split(jax.random.key(seed), 3)
    signal = draw_signal(jax.random.fold_in(arg_keys[2], 71), 0)
    tap_gain = jnp.clip(jax.random.uniform(arg_keys[1], (3, CHANNELS), jnp.float32, 0.3, 1.2), 0.3, 1.2)
    return {"signal": signal, "tap_gain": tap_gain}


def reference(signal, tap_gain):
    wide_in = signal.astype(jnp.float32)
    mixed = tap_gain[0] * wide_in + tap_gain[1] * jnp.roll(wide_in, 2, axis=0) + tap_gain[2] * jnp.roll(wide_in, 3, axis=0)
    power = lax.optimization_barrier(jnp.mean(mixed * mixed, axis=(0, 2), keepdims=True))
    echoed = (mixed * lax.rsqrt(power + 1e-05)).astype(jnp.bfloat16)
    return echoed
```

```python
import functools

import jax
import jax.numpy as jnp
from jax import lax
from jax.experimental import pallas as pl
from jax.experimental.pallas import tpu as pltpu
from jax.sharding import PartitionSpec as P

MESH = pl.DeviceIdType.MESH
X = 4
PIECES = 16
LAG = 1
EARLY = 8
BLOCK = 16
MIB = 2**20


def kernel(
    sig, gain, out, mine, row, below, mixed, back, acc, part_x, part_y, sum_y,
    load_sem, in_send, in_recv, up_send, up_recv, out_send, out_recv,
    py_send, py_recv, px_send, px_recv,
):
    me = lax.axis_index("phase")
    phases = lax.axis_size("phase")
    Y = phases // X
    x, y = lax.rem(me, X), me // X
    steps = row.shape[1]
    R = steps // PIECES

    def along_x(d):
        return lax.rem(x + d, X)

    def along_y(d):
        return lax.rem(y + d, Y)

    def quarter(c):
        return sig.at[pl.ds(pl.multiple_of(c * steps, steps), steps)]

    loads = [pltpu.make_async_copy(quarter(along_x(d)), mine.at[d - 1], load_sem.at[d]) for d in range(1, X)]
    loads.append(pltpu.make_async_copy(quarter(x), row.at[x], load_sem.at[0]))
    for load in loads:
        load.start()

    barrier = pltpu.get_barrier_semaphore()
    for d in range(1, X):
        pl.semaphore_signal(barrier, inc=1, device_id={"phase": y * X + along_x(d)}, device_id_type=MESH)
    for d in range(1, Y):
        pl.semaphore_signal(barrier, inc=1, device_id={"phase": along_y(d) * X + x}, device_id_type=MESH)
    pl.semaphore_wait(barrier, X + Y - 2)
    for load in loads:
        load.wait()

    def piece(k):
        return pl.ds(pl.multiple_of(k * R, R), R)

    def send_in(d, k):
        return pltpu.make_async_remote_copy(
            src_ref=mine.at[d - 1, piece(k)],
            dst_ref=row.at[x, piece(k)],
            send_sem=in_send.at[d - 1],
            recv_sem=in_recv.at[x, k],
            device_id={"phase": y * X + along_x(d)},
            device_id_type=MESH,
        )

    def wait_in(c, k):
        pltpu.make_async_copy(row.at[c, piece(k)], row.at[c, piece(k)], in_recv.at[c, k]).wait()

    def send_up(c, k):
        return pltpu.make_async_remote_copy(
            src_ref=row.at[c, piece(k)],
            dst_ref=below.at[c - 1, piece(k)],
            send_sem=up_send.at[c - 1],
            recv_sem=up_recv.at[c - 1, k],
            device_id={"phase": along_y(1) * X + x},
            device_id_type=MESH,
        )

    def send_out(d, k):
        c = along_x(d)
        return pltpu.make_async_remote_copy(
            src_ref=mixed.at[c, piece(k)],
            dst_ref=back.at[x, piece(k)],
            send_sem=out_send.at[d - 1],
            recv_sem=out_recv.at[x, k],
            device_id={"phase": y * X + c},
            device_id_type=MESH,
        )

    def wait_out(c, k):
        pltpu.make_async_copy(back.at[c, piece(k)], back.at[c, piece(k)], out_recv.at[c, k]).wait()

    @pl.loop(0, PIECES)
    def _(k):
        for d in (2, 1, 3):
            send_in(d, k).start()

    acc[...] = jnp.zeros_like(acc)

    def gather(k):
        for d in (1, 3, 2):
            wait_in(along_x(d), k)
        for c in range(1, X):
            send_up(c, k).start()

    def mix(k):
        for c in range(1, X):
            send_up(c, k).wait_recv()
        g0, g1, g2 = (jnp.broadcast_to(gain[i : i + 1, :], (8, gain.shape[1])) for i in range(3))

        def block(i, total):
            rows = pl.ds(pl.multiple_of(k * R + i * BLOCK, BLOCK), BLOCK)
            taps = [below[c, rows, :] for c in range(X - 1)] + [row[c, rows, :] for c in range(X)]
            taps = [t.astype(jnp.float32).reshape(BLOCK // 8, 8, -1) for t in taps]
            for c in range(X):
                m = g0 * taps[c + 3] + g1 * taps[c + 1] + g2 * taps[c]
                total = total + jnp.sum(m * m, axis=0)
                mixed[c, rows, :] = m.reshape(BLOCK, -1).astype(jnp.bfloat16)
            return total

        acc[...] = lax.fori_loop(0, R // BLOCK, block, acc[...])

    def give_back(k):
        for d in (2, 1, 3):
            send_out(d, k).start()

    @pl.loop(0, LAG)
    def _(k):
        gather(k)

    @pl.loop(LAG, EARLY + LAG)
    def _(k):
        gather(k)
        mix(k - LAG)
        give_back(k - LAG)

    @pl.loop(EARLY + LAG, PIECES)
    def _(k):
        gather(k)
        mix(k - LAG)

    @pl.loop(PIECES - LAG, PIECES)
    def _(k):
        mix(k)

    def power_y(d):
        return pltpu.make_async_remote_copy(
            src_ref=acc, dst_ref=part_y.at[y], send_sem=py_send.at[d - 1], recv_sem=py_recv.at[y],
            device_id={"phase": along_y(d) * X + x}, device_id_type=MESH,
        )

    def power_x(d):
        return pltpu.make_async_remote_copy(
            src_ref=sum_y, dst_ref=part_x.at[x], send_sem=px_send.at[d - 1], recv_sem=px_recv.at[x],
            device_id={"phase": y * X + along_x(d)}, device_id_type=MESH,
        )

    for d in range(1, Y):
        power_y(d).start()
    total = acc[...]
    for d in range(1, Y):
        r = along_y(d)
        pltpu.make_async_copy(part_y.at[r], part_y.at[r], py_recv.at[r]).wait()
        total = total + part_y[r]
    sum_y[...] = total
    for d in range(1, X):
        power_x(d).start()

    @pl.loop(EARLY, PIECES)
    def _(k):
        give_back(k)

    total = sum_y[...]
    for d in range(1, X):
        c = along_x(d)
        pltpu.make_async_copy(part_x.at[c], part_x.at[c], px_recv.at[c]).wait()
        total = total + part_x[c]
    count = X * steps * phases
    power = jnp.sum(total, axis=0, keepdims=True) / count
    scale = jnp.broadcast_to(lax.rsqrt(power + 1e-05), (BLOCK, out.shape[1]))

    def finish(source, c, k):
        @pl.loop(0, R // BLOCK)
        def _(i):
            rows = pl.multiple_of(k * R + i * BLOCK, BLOCK)
            m = source[c, pl.ds(rows, BLOCK), :].astype(jnp.float32)
            out[pl.ds(pl.multiple_of(c * steps + rows, BLOCK), BLOCK), :] = (m * scale).astype(jnp.bfloat16)

    @pl.loop(0, PIECES)
    def _(k):
        finish(mixed, x, k)

    @pl.loop(0, PIECES)
    def _(k):
        for d in (1, 3, 2):
            c = along_x(d)
            wait_out(c, k)
            finish(back, c, k)

    for d in range(1, X):
        pltpu.make_async_copy(mine.at[d - 1], mine.at[d - 1], in_send.at[d - 1]).wait()
        pltpu.make_async_copy(row.at[d], row.at[d], up_send.at[d - 1]).wait()
        c = along_x(d)
        pltpu.make_async_copy(mixed.at[c], mixed.at[c], out_send.at[d - 1]).wait()
        power_x(d).wait_send()
    for d in range(1, Y):
        power_y(d).wait_send()


def body(signal, tap_gain):
    steps, channels = signal.shape[2:]
    phases = lax.axis_size("phase")
    Y = phases // X
    part = steps // X
    dma = pltpu.SemaphoreType.DMA
    out = pl.pallas_call(
        kernel,
        name="echoes",
        out_shape=jax.ShapeDtypeStruct((steps, channels), signal.dtype),
        in_specs=[pl.BlockSpec(memory_space=pltpu.HBM), pl.BlockSpec(memory_space=pltpu.VMEM)],
        out_specs=pl.BlockSpec(memory_space=pltpu.VMEM),
        scratch_shapes=[
            pltpu.VMEM((X - 1, part, channels), jnp.bfloat16),
            pltpu.VMEM((X, part, channels), jnp.bfloat16),
            pltpu.VMEM((X - 1, part, channels), jnp.bfloat16),
            pltpu.VMEM((X, part, channels), jnp.bfloat16),
            pltpu.VMEM((X, part, channels), jnp.bfloat16),
            pltpu.VMEM((8, channels), jnp.float32),
            pltpu.VMEM((X, 8, channels), jnp.float32),
            pltpu.VMEM((Y, 8, channels), jnp.float32),
            pltpu.VMEM((8, channels), jnp.float32),
            dma((X,)),
            dma((X - 1,)),
            dma((X, PIECES)),
            dma((X - 1,)),
            dma((X - 1, PIECES)),
            dma((X - 1,)),
            dma((X, PIECES)),
            dma((Y - 1,)),
            dma((Y,)),
            dma((X - 1,)),
            dma((X,)),
        ],
        compiler_params=pltpu.CompilerParams(
            collective_id=0, has_side_effects=True, vmem_limit_bytes=40 * MIB
        ),
    )(signal.reshape(steps, channels), tap_gain)
    return out.reshape(signal.shape)


def solution(mesh):
    return jax.shard_map(
        body,
        mesh=mesh,
        in_specs=(P("phase", "line", None, None), P()),
        out_specs=P("phase", "line", None, None),
        check_vma=False,
    )
```

```python
import functools

import jax
import jax.numpy as jnp
from jax import lax
from jax.experimental import pallas as pl
from jax.experimental.pallas import tpu as pltpu
from jax.sharding import PartitionSpec as P

MESH = pl.DeviceIdType.MESH
X = 4
PIECES = 16
LAG = 1
EARLY = 12
BLOCK = 16
MIB = 2**20
VMEM = 54 * MIB


def kernel(
    sig, gain, out, mine, row, below, mixed, back, acc, part_x, part_y, sum_y,
    load_sem, in_send, in_recv, up_send, up_recv, out_send, out_recv,
    py_send, py_recv, px_send, px_recv,
):
    me = lax.axis_index("phase")
    phases = lax.axis_size("phase")
    Y = phases // X
    x, y = lax.rem(me, X), me // X
    steps = row.shape[1]
    R = steps // PIECES

    def along_x(d):
        return lax.rem(x + d, X)

    def along_y(d):
        return lax.rem(y + d, Y)

    def quarter(c):
        return sig.at[pl.ds(pl.multiple_of(c * steps, steps), steps)]

    loads = [pltpu.make_async_copy(quarter(along_x(d)), mine.at[d - 1], load_sem.at[d]) for d in range(1, X)]
    loads.append(pltpu.make_async_copy(quarter(x), row.at[x], load_sem.at[0]))
    for load in loads:
        load.start()

    barrier = pltpu.get_barrier_semaphore()
    for d in range(1, X):
        pl.semaphore_signal(barrier, inc=1, device_id={"phase": y * X + along_x(d)}, device_id_type=MESH)
    for d in range(1, Y):
        pl.semaphore_signal(barrier, inc=1, device_id={"phase": along_y(d) * X + x}, device_id_type=MESH)
    pl.semaphore_wait(barrier, X + Y - 2)
    for load in loads:
        load.wait()

    def piece(k):
        return pl.ds(pl.multiple_of(k * R, R), R)

    def send_in(d, k):
        return pltpu.make_async_remote_copy(
            src_ref=mine.at[d - 1, piece(k)],
            dst_ref=row.at[x, piece(k)],
            send_sem=in_send.at[d - 1],
            recv_sem=in_recv.at[x, k],
            device_id={"phase": y * X + along_x(d)},
            device_id_type=MESH,
        )

    def wait_in(c, k):
        pltpu.make_async_copy(row.at[c, piece(k)], row.at[c, piece(k)], in_recv.at[c, k]).wait()

    def send_up(c, k):
        return pltpu.make_async_remote_copy(
            src_ref=row.at[c, piece(k)],
            dst_ref=below.at[c - 1, piece(k)],
            send_sem=up_send.at[c - 1],
            recv_sem=up_recv.at[c - 1, k],
            device_id={"phase": along_y(1) * X + x},
            device_id_type=MESH,
        )

    def send_out(d, k):
        c = along_x(d)
        return pltpu.make_async_remote_copy(
            src_ref=mixed.at[c, piece(k)],
            dst_ref=back.at[x, piece(k)],
            send_sem=out_send.at[d - 1],
            recv_sem=out_recv.at[x, k],
            device_id={"phase": y * X + c},
            device_id_type=MESH,
        )

    def wait_out(c, k):
        pltpu.make_async_copy(back.at[c, piece(k)], back.at[c, piece(k)], out_recv.at[c, k]).wait()

    @pl.loop(0, PIECES)
    def _(k):
        for d in (2, 1, 3):
            send_in(d, k).start()

    acc[...] = jnp.zeros_like(acc)

    def gather(k):
        for d in (1, 3, 2):
            wait_in(along_x(d), k)
        for c in range(1, X):
            send_up(c, k).start()

    def mix(k):
        for c in range(1, X):
            send_up(c, k).wait_recv()
        g0, g1, g2 = (jnp.broadcast_to(gain[i : i + 1, :], (8, gain.shape[1])) for i in range(3))

        def block(i, total):
            rows = pl.ds(pl.multiple_of(k * R + i * BLOCK, BLOCK), BLOCK)
            taps = [below[c, rows, :] for c in range(X - 1)] + [row[c, rows, :] for c in range(X)]
            taps = [t.astype(jnp.float32).reshape(BLOCK // 8, 8, -1) for t in taps]
            for c in range(X):
                m = g0 * taps[c + 3] + g1 * taps[c + 1] + g2 * taps[c]
                total = total + jnp.sum(m * m, axis=0)
                mixed[c, rows, :] = m.reshape(BLOCK, -1).astype(jnp.bfloat16)
            return total

        acc[...] = lax.fori_loop(0, R // BLOCK, block, acc[...])

    def give_back(k):
        for d in (2, 1, 3):
            send_out(d, k).start()

    def stage(start, stop, *, first=True, second=True, third=True):
        if start < stop:

            @pl.loop(start, stop)
            def _(k):
                if first:
                    gather(k)
                if second:
                    mix(k - LAG)
                if second and third:
                    give_back(k - LAG)

    turn = min(EARLY + LAG, PIECES)
    stage(0, LAG, second=False)
    stage(LAG, turn)
    stage(turn, PIECES, third=False)
    stage(PIECES, EARLY + LAG, first=False)
    stage(max(PIECES, EARLY + LAG), PIECES + LAG, first=False, third=False)

    def power_y(d):
        return pltpu.make_async_remote_copy(
            src_ref=acc, dst_ref=part_y.at[y], send_sem=py_send.at[d - 1], recv_sem=py_recv.at[y],
            device_id={"phase": along_y(d) * X + x}, device_id_type=MESH,
        )

    def power_x(d):
        return pltpu.make_async_remote_copy(
            src_ref=sum_y, dst_ref=part_x.at[x], send_sem=px_send.at[d - 1], recv_sem=px_recv.at[x],
            device_id={"phase": y * X + along_x(d)}, device_id_type=MESH,
        )

    for d in range(1, Y):
        power_y(d).start()
    total = acc[...]
    for d in range(1, Y):
        r = along_y(d)
        pltpu.make_async_copy(part_y.at[r], part_y.at[r], py_recv.at[r]).wait()
        total = total + part_y[r]
    sum_y[...] = total
    for d in range(1, X):
        power_x(d).start()

    @pl.loop(EARLY, PIECES)
    def _(k):
        give_back(k)

    total = sum_y[...]
    for d in range(1, X):
        c = along_x(d)
        pltpu.make_async_copy(part_x.at[c], part_x.at[c], px_recv.at[c]).wait()
        total = total + part_x[c]
    count = X * steps * phases
    power = jnp.sum(total, axis=0, keepdims=True) / count
    scale = jnp.broadcast_to(lax.rsqrt(power + 1e-05), (BLOCK, out.shape[1]))

    def finish(source, c, k):
        @pl.loop(0, R // BLOCK)
        def _(i):
            rows = pl.multiple_of(k * R + i * BLOCK, BLOCK)
            m = source[c, pl.ds(rows, BLOCK), :].astype(jnp.float32)
            out[pl.ds(pl.multiple_of(c * steps + rows, BLOCK), BLOCK), :] = (m * scale).astype(jnp.bfloat16)

    @pl.loop(0, PIECES)
    def _(k):
        finish(mixed, x, k)

    @pl.loop(0, PIECES)
    def _(k):
        for d in (1, 3, 2):
            c = along_x(d)
            wait_out(c, k)
            finish(back, c, k)

    for d in range(1, X):
        pltpu.make_async_copy(mine.at[d - 1], mine.at[d - 1], in_send.at[d - 1]).wait()
        pltpu.make_async_copy(row.at[d], row.at[d], up_send.at[d - 1]).wait()
        c = along_x(d)
        pltpu.make_async_copy(mixed.at[c], mixed.at[c], out_send.at[d - 1]).wait()
        power_x(d).wait_send()
    for d in range(1, Y):
        power_y(d).wait_send()


def body(signal, tap_gain):
    steps, channels = signal.shape[2:]
    phases = lax.axis_size("phase")
    Y = phases // X
    part = steps // X
    dma = pltpu.SemaphoreType.DMA
    out = pl.pallas_call(
        kernel,
        name="echoes",
        out_shape=pltpu.VMEM((steps, channels), signal.dtype),
        in_specs=[pl.BlockSpec(memory_space=pltpu.HBM), pl.BlockSpec(memory_space=pltpu.VMEM)],
        out_specs=pl.BlockSpec(memory_space=pltpu.VMEM),
        scratch_shapes=[
            pltpu.VMEM((X - 1, part, channels), jnp.bfloat16),
            pltpu.VMEM((X, part, channels), jnp.bfloat16),
            pltpu.VMEM((X - 1, part, channels), jnp.bfloat16),
            pltpu.VMEM((X, part, channels), jnp.bfloat16),
            pltpu.VMEM((X, part, channels), jnp.bfloat16),
            pltpu.VMEM((8, channels), jnp.float32),
            pltpu.VMEM((X, 8, channels), jnp.float32),
            pltpu.VMEM((Y, 8, channels), jnp.float32),
            pltpu.VMEM((8, channels), jnp.float32),
            dma((X,)),
            dma((X - 1,)),
            dma((X, PIECES)),
            dma((X - 1,)),
            dma((X - 1, PIECES)),
            dma((X - 1,)),
            dma((X, PIECES)),
            dma((Y - 1,)),
            dma((Y,)),
            dma((X - 1,)),
            dma((X,)),
        ],
        compiler_params=pltpu.CompilerParams(
            collective_id=0, has_side_effects=True, vmem_limit_bytes=VMEM
        ),
    )(signal.reshape(steps, channels), tap_gain)
    return out.reshape(signal.shape)


def solution(mesh):
    return jax.shard_map(
        body,
        mesh=mesh,
        in_specs=(P("phase", "line", None, None), P()),
        out_specs=P("phase", "line", None, None),
        check_vma=False,
    )
```

```python
import jax
import jax.numpy as jnp
from jax import lax
from jax.experimental import pallas as pl
from jax.experimental.pallas import tpu as pltpu
from jax.sharding import PartitionSpec as P

MESH = pl.DeviceIdType.MESH
X = 4
PIECES = 16
LAG = 1
EARLY = 12
LEAD = 2
BLOCK = 16
WIDE = 64
MIB = 2**20
VMEM = 54 * MIB


def kernel(
    sig, gain_in, out, gain, mine, row, below, mixed, back, acc, part_x, part_y, sum_y,
    load_sem, in_send, in_recv, up_send, up_recv, out_send, out_recv, power_send, power_recv,
):
    me = lax.axis_index("phase")
    phases = lax.axis_size("phase")
    Y = phases // X
    x, y = lax.rem(me, X), me // X
    steps = row.shape[1]
    R = steps // PIECES

    def along_x(d):
        return lax.rem(x + d, X)

    def along_y(d):
        return lax.rem(y + d, Y)

    def at_x(c):
        return {"phase": y * X + c}

    def at_y(r):
        return {"phase": r * X + x}

    def piece(k, count=1):
        return pl.ds(pl.multiple_of(k * R, R), count * R)

    def wait_for(ref, sem):
        pltpu.make_async_copy(ref, ref, sem).wait()

    barrier = pltpu.get_barrier_semaphore()
    for d in range(1, X):
        pl.semaphore_signal(barrier, inc=1, device_id=at_x(along_x(d)), device_id_type=MESH)
    for d in range(1, Y):
        pl.semaphore_signal(barrier, inc=1, device_id=at_y(along_y(d)), device_id_type=MESH)

    first, rest = piece(0, LEAD), piece(LEAD, PIECES - LEAD)
    loads = [
        pltpu.make_async_copy(sig.at[:, first], mine.at[:, first], load_sem.at[0]),
        pltpu.make_async_copy(sig.at[:, rest], mine.at[:, rest], load_sem.at[1]),
        pltpu.make_async_copy(sig.at[x], row.at[x], load_sem.at[2]),
        pltpu.make_async_copy(gain_in, gain, load_sem.at[3]),
    ]
    for load in loads:
        load.start()
    acc[...] = jnp.zeros_like(acc)
    pl.semaphore_wait(barrier, X + Y - 2)

    def send_in(c, k):
        @pl.when(x != c)
        def _():
            pltpu.make_async_remote_copy(
                src_ref=mine.at[c, piece(k)],
                dst_ref=row.at[x, piece(k)],
                send_sem=in_send,
                recv_sem=in_recv.at[k],
                device_id=at_x(c),
                device_id_type=MESH,
            ).start()

    def send_up(c, k):
        pltpu.make_async_remote_copy(
            src_ref=row.at[c, piece(k)],
            dst_ref=below.at[c - 1, piece(k)],
            send_sem=up_send,
            recv_sem=up_recv.at[k],
            device_id=at_y(along_y(1)),
            device_id_type=MESH,
        ).start()

    def send_out(d, k):
        c = along_x(d)
        pltpu.make_async_remote_copy(
            src_ref=mixed.at[c, piece(k)],
            dst_ref=back.at[x, piece(k)],
            send_sem=out_send,
            recv_sem=out_recv.at[k],
            device_id=at_x(c),
            device_id_type=MESH,
        ).start()

    def three(ref, k):
        return ref.at[: X - 1, piece(k)]

    loads[0].wait()
    for k in range(LEAD):
        send_in(0, k)
    for k in range(LEAD):
        for c in (2, 1, 3):
            send_in(c, k)
    loads[1].wait()

    @pl.loop(LEAD, PIECES)
    def _(k):
        for c in (0, 2, 1, 3):
            send_in(c, k)

    loads[2].wait()

    @pl.when(x > 0)
    def _():
        @pl.loop(0, PIECES)
        def _(k):
            send_up(x, k)

    loads[3].wait()

    def gather(k):
        wait_for(three(row, k), in_recv.at[k])
        for c in range(1, X):

            @pl.when(x != c)
            def _(c=c):
                send_up(c, k)

    def mix(k):
        wait_for(three(below, k), up_recv.at[k])
        g0, g1, g2 = (jnp.broadcast_to(gain[i : i + 1, :], (8, gain.shape[1])) for i in range(3))

        def block(i, total):
            rows = pl.ds(pl.multiple_of(k * R + i * BLOCK, BLOCK), BLOCK)
            taps = [below[c, rows, :] for c in range(X - 1)] + [row[c, rows, :] for c in range(X)]
            taps = [t.astype(jnp.float32).reshape(BLOCK // 8, 8, -1) for t in taps]
            for c in range(X):
                m = g0 * taps[c + 3] + g1 * taps[c + 1] + g2 * taps[c]
                total = total + jnp.sum(m * m, axis=0)
                mixed[c, rows, :] = m.reshape(BLOCK, -1).astype(jnp.bfloat16)
            return total

        acc[...] = lax.fori_loop(0, R // BLOCK, block, acc[...])

    def give_back(k):
        for d in (2, 1, 3):
            send_out(d, k)

    def stage(start, stop, *, first=True, second=True, third=True):
        if start < stop:

            @pl.loop(start, stop)
            def _(k):
                if first:
                    gather(k)
                if second:
                    mix(k - LAG)
                if second and third:
                    give_back(k - LAG)

    turn = min(EARLY + LAG, PIECES)
    stage(0, LAG, second=False)
    stage(LAG, turn)
    stage(turn, PIECES, third=False)
    stage(PIECES, EARLY + LAG, first=False)
    stage(max(PIECES, EARLY + LAG), PIECES + LAG, first=False, third=False)

    for d in range(1, Y):
        pltpu.make_async_remote_copy(
            src_ref=acc, dst_ref=part_y.at[d - 1], send_sem=power_send.at[0], recv_sem=power_recv.at[0],
            device_id=at_y(along_y(d)), device_id_type=MESH,
        ).start()
    wait_for(part_y, power_recv.at[0])
    sum_y[...] = acc[...] + jnp.sum(part_y[...], axis=0)
    for d in range(1, X):
        pltpu.make_async_remote_copy(
            src_ref=sum_y, dst_ref=part_x.at[d - 1], send_sem=power_send.at[1], recv_sem=power_recv.at[1],
            device_id=at_x(along_x(d)), device_id_type=MESH,
        ).start()

    @pl.loop(EARLY, PIECES)
    def _(k):
        give_back(k)

    wait_for(part_x, power_recv.at[1])
    total = sum_y[...] + jnp.sum(part_x[...], axis=0)
    power = jnp.sum(total, axis=0, keepdims=True) / (X * steps * phases)
    scale = jnp.broadcast_to(lax.rsqrt(power + 1e-05), (8, out.shape[2]))

    def finish(source, c, start, stop):
        @pl.loop(start // WIDE, stop // WIDE)
        def _(i):
            rows = pl.ds(pl.multiple_of(i * WIDE, WIDE), WIDE)
            m = source[c, rows, :].astype(jnp.float32).reshape(WIDE // 8, 8, -1) * scale
            out[c, rows, :] = m.reshape(WIDE, -1).astype(jnp.bfloat16)

    finish(mixed, x, 0, steps)

    @pl.loop(0, PIECES)
    def _(k):
        wait_for(three(back, k), out_recv.at[k])
        for d in range(1, X):
            finish(back, along_x(d), k * R, (k + 1) * R)

    wait_for(mine.at[: X - 1], in_send)
    wait_for(below, up_send)
    wait_for(mixed.at[: X - 1], out_send)
    wait_for(part_y, power_send.at[0])
    wait_for(part_x, power_send.at[1])


def body(signal, tap_gain):
    steps, channels = signal.shape[2:]
    Y = lax.axis_size("phase") // X
    part = steps // X
    dma = pltpu.SemaphoreType.DMA

    def rows(n):
        return pltpu.VMEM((n, part, channels), jnp.bfloat16)

    def sums(*n):
        return pltpu.VMEM((*n, 8, channels), jnp.float32)

    out = pl.pallas_call(
        kernel,
        name="echoes",
        out_shape=pltpu.VMEM((X, part, channels), signal.dtype),
        in_specs=[pl.BlockSpec(memory_space=pltpu.HBM)] * 2,
        out_specs=pl.BlockSpec(memory_space=pltpu.VMEM),
        scratch_shapes=[
            pltpu.VMEM(tap_gain.shape, jnp.float32),
            rows(X),
            rows(X),
            rows(X - 1),
            rows(X),
            rows(X),
            sums(),
            sums(X - 1),
            sums(Y - 1),
            sums(),
            dma((4,)),
            dma(()),
            dma((PIECES,)),
            dma(()),
            dma((PIECES,)),
            dma(()),
            dma((PIECES,)),
            dma((2,)),
            dma((2,)),
        ],
        compiler_params=pltpu.CompilerParams(
            collective_id=0, has_side_effects=True, vmem_limit_bytes=VMEM
        ),
    )(signal.reshape(X, part, channels), tap_gain)
    return out.reshape(signal.shape)


def solution(mesh):
    return jax.shard_map(
        body,
        mesh=mesh,
        in_specs=(P("phase", "line", None, None), P()),
        out_specs=P("phase", "line", None, None),
        check_vma=False,
    )
```

```python
import jax
import jax.numpy as jnp
from jax import lax
from jax.experimental import pallas as pl
from jax.experimental.pallas import tpu as pltpu
from jax.sharding import PartitionSpec as P

MESH = pl.DeviceIdType.MESH
X = 4
PIECES = 16
LAG = 1
EARLY = 12
LEAD = 2
BLOCK = 16
WIDE = 64
MIB = 2**20
VMEM = 54 * MIB


def kernel(
    sig, gain_in, out, gain, mine, row, below, mixed, back, acc, part_x, part_y, sum_y,
    ready, load_sem, in_send, in_recv, up_send, up_recv, out_send, out_recv, power_send, power_recv,
):
    me = lax.axis_index("phase")
    phases = lax.axis_size("phase")
    Y = phases // X
    x, y = lax.rem(me, X), me // X
    steps = row.shape[1]
    R = steps // PIECES

    def along_x(d):
        return lax.rem(x + d, X)

    def along_y(d):
        return lax.rem(y + d, Y)

    def at_x(c):
        return {"phase": y * X + c}

    def at_y(r):
        return {"phase": r * X + x}

    def piece(k, count=1):
        return pl.ds(pl.multiple_of(k * R, R), count * R)

    def wait_for(ref, sem):
        pltpu.make_async_copy(ref, ref, sem).wait()

    barrier = pltpu.get_barrier_semaphore()
    for peer in (at_x(along_x(X - 1)), at_x(along_x(1)), at_y(along_y(Y - 1))):
        pl.semaphore_signal(barrier, inc=1, device_id=peer, device_id_type=MESH)

    first, rest = piece(0, LEAD), piece(LEAD, PIECES - LEAD)
    loads = [
        pltpu.make_async_copy(sig.at[:, first], mine.at[:, first], load_sem.at[0]),
        pltpu.make_async_copy(sig.at[:, rest], mine.at[:, rest], load_sem.at[1]),
        pltpu.make_async_copy(sig.at[x], row.at[x], load_sem.at[2]),
        pltpu.make_async_copy(gain_in, gain, load_sem.at[3]),
    ]
    for load in loads:
        load.start()
    acc[...] = jnp.zeros_like(acc)
    pl.semaphore_wait(barrier, 3)
    pl.semaphore_signal(ready, inc=1, device_id=at_x(along_x(X - 1)), device_id_type=MESH)

    def send_in(c, k):
        pltpu.make_async_remote_copy(
            src_ref=mine.at[c, piece(k)],
            dst_ref=row.at[x, piece(k)],
            send_sem=in_send,
            recv_sem=in_recv.at[k],
            device_id=at_x(c),
            device_id_type=MESH,
        ).start()

    def send_up(c, k):
        pltpu.make_async_remote_copy(
            src_ref=row.at[c, piece(k)],
            dst_ref=below.at[c - 1, piece(k)],
            send_sem=up_send,
            recv_sem=up_recv.at[k],
            device_id=at_y(along_y(1)),
            device_id_type=MESH,
        ).start()

    def send_out(d, k):
        c = along_x(d)
        pltpu.make_async_remote_copy(
            src_ref=mixed.at[c, piece(k)],
            dst_ref=back.at[x, piece(k)],
            send_sem=out_send,
            recv_sem=out_recv.at[k],
            device_id=at_x(c),
            device_id_type=MESH,
        ).start()

    def three(ref, k):
        return ref.at[: X - 1, piece(k)]

    loads[0].wait()
    for k in range(LEAD):
        send_in(along_x(1), k)
        send_in(along_x(3), k)
    pl.semaphore_wait(ready, 1)
    for k in range(LEAD):
        send_in(along_x(2), k)
    loads[1].wait()

    @pl.loop(LEAD, PIECES)
    def _(k):
        for c in (0, 2, 1, 3):

            @pl.when(x != c)
            def _(c=c):
                send_in(c, k)

    loads[2].wait()

    @pl.when(x > 0)
    def _():
        @pl.loop(0, PIECES)
        def _(k):
            send_up(x, k)

    loads[3].wait()

    def gather(k):
        wait_for(three(row, k), in_recv.at[k])
        for c in range(1, X):

            @pl.when(x != c)
            def _(c=c):
                send_up(c, k)

    def mix(k):
        wait_for(three(below, k), up_recv.at[k])
        g0, g1, g2 = (jnp.broadcast_to(gain[i : i + 1, :], (8, gain.shape[1])) for i in range(3))

        def block(i, total):
            rows = pl.ds(pl.multiple_of(k * R + i * BLOCK, BLOCK), BLOCK)
            taps = [below[c, rows, :] for c in range(X - 1)] + [row[c, rows, :] for c in range(X)]
            taps = [t.astype(jnp.float32).reshape(BLOCK // 8, 8, -1) for t in taps]
            for c in range(X):
                m = g0 * taps[c + 3] + g1 * taps[c + 1] + g2 * taps[c]
                total = total + jnp.sum(m * m, axis=0)
                mixed[c, rows, :] = m.reshape(BLOCK, -1).astype(jnp.bfloat16)
            return total

        acc[...] = lax.fori_loop(0, R // BLOCK, block, acc[...])

    def give_back(k):
        for d in (2, 1, 3):
            send_out(d, k)

    def stage(start, stop, *, first=True, second=True, third=True):
        if start < stop:

            @pl.loop(start, stop)
            def _(k):
                if first:
                    gather(k)
                if second:
                    mix(k - LAG)
                if second and third:
                    give_back(k - LAG)

    turn = min(EARLY + LAG, PIECES)
    stage(0, LAG, second=False)
    stage(LAG, turn)
    stage(turn, PIECES, third=False)
    stage(PIECES, EARLY + LAG, first=False)
    stage(max(PIECES, EARLY + LAG), PIECES + LAG, first=False, third=False)

    for d in range(1, Y):
        pltpu.make_async_remote_copy(
            src_ref=acc, dst_ref=part_y.at[d - 1], send_sem=power_send.at[0], recv_sem=power_recv.at[0],
            device_id=at_y(along_y(d)), device_id_type=MESH,
        ).start()
    wait_for(part_y, power_recv.at[0])
    sum_y[...] = acc[...] + jnp.sum(part_y[...], axis=0)
    for d in range(1, X):
        pltpu.make_async_remote_copy(
            src_ref=sum_y, dst_ref=part_x.at[d - 1], send_sem=power_send.at[1], recv_sem=power_recv.at[1],
            device_id=at_x(along_x(d)), device_id_type=MESH,
        ).start()

    @pl.loop(EARLY, PIECES)
    def _(k):
        give_back(k)

    wait_for(part_x, power_recv.at[1])
    total = sum_y[...] + jnp.sum(part_x[...], axis=0)
    power = jnp.sum(total, axis=0, keepdims=True) / (X * steps * phases)
    scale = jnp.broadcast_to(lax.rsqrt(power + 1e-05), (8, out.shape[2]))

    def finish(source, c, start, stop):
        @pl.loop(start // WIDE, stop // WIDE)
        def _(i):
            rows = pl.ds(pl.multiple_of(i * WIDE, WIDE), WIDE)
            m = source[c, rows, :].astype(jnp.float32).reshape(WIDE // 8, 8, -1) * scale
            out[c, rows, :] = m.reshape(WIDE, -1).astype(jnp.bfloat16)

    finish(mixed, x, 0, steps)

    @pl.loop(0, PIECES)
    def _(k):
        wait_for(three(back, k), out_recv.at[k])
        for d in range(1, X):
            finish(back, along_x(d), k * R, (k + 1) * R)

    wait_for(mine.at[: X - 1], in_send)
    wait_for(below, up_send)
    wait_for(mixed.at[: X - 1], out_send)
    wait_for(part_y, power_send.at[0])
    wait_for(part_x, power_send.at[1])


def body(signal, tap_gain):
    steps, channels = signal.shape[2:]
    Y = lax.axis_size("phase") // X
    part = steps // X
    dma = pltpu.SemaphoreType.DMA

    def rows(n):
        return pltpu.VMEM((n, part, channels), jnp.bfloat16)

    def sums(*n):
        return pltpu.VMEM((*n, 8, channels), jnp.float32)

    out = pl.pallas_call(
        kernel,
        name="echoes",
        out_shape=pltpu.VMEM((X, part, channels), signal.dtype),
        in_specs=[pl.BlockSpec(memory_space=pltpu.HBM)] * 2,
        out_specs=pl.BlockSpec(memory_space=pltpu.VMEM),
        scratch_shapes=[
            pltpu.VMEM(tap_gain.shape, jnp.float32),
            rows(X),
            rows(X),
            rows(X - 1),
            rows(X),
            rows(X),
            sums(),
            sums(X - 1),
            sums(Y - 1),
            sums(),
            pltpu.SemaphoreType.REGULAR,
            dma((4,)),
            dma(()),
            dma((PIECES,)),
            dma(()),
            dma((PIECES,)),
            dma(()),
            dma((PIECES,)),
            dma((2,)),
            dma((2,)),
        ],
        compiler_params=pltpu.CompilerParams(
            collective_id=0, has_side_effects=True, vmem_limit_bytes=VMEM
        ),
    )(signal.reshape(X, part, channels), tap_gain)
    return out.reshape(signal.shape)


def solution(mesh):
    return jax.shard_map(
        body,
        mesh=mesh,
        in_specs=(P("phase", "line", None, None), P()),
        out_specs=P("phase", "line", None, None),
        check_vma=False,
    )
```

```python
import jax
import jax.numpy as jnp
from jax import lax
from jax.experimental import pallas as pl
from jax.experimental.pallas import tpu as pltpu
from jax.sharding import PartitionSpec as P

MESH = pl.DeviceIdType.MESH
X = 4
PIECES = 8
LAG = 1
EARLY = (7, 5)
LEAD = 1
BLOCK = 16
WIDE = 64
MIB = 2**20
VMEM = 54 * MIB


def kernel(
    sig, gain_in, out, gain, mine, row, below, mixed, back, acc, part_x, part_y, sum_y,
    ready, load_sem, in_send, in_recv, up_send, up_recv, out_send, out_recv, power_send, power_recv,
):
    me = lax.axis_index("phase")
    phases = lax.axis_size("phase")
    Y = phases // X
    x, y = lax.rem(me, X), me // X
    steps = row.shape[1]
    R = steps // PIECES

    def along_x(d):
        return lax.rem(x + d, X)

    def along_y(d):
        return lax.rem(y + d, Y)

    def at_x(c):
        return {"phase": y * X + c}

    def at_y(r):
        return {"phase": r * X + x}

    def piece(k, count=1):
        return pl.ds(pl.multiple_of(k * R, R), count * R)

    def wait_for(ref, sem):
        pltpu.make_async_copy(ref, ref, sem).wait()

    barrier = pltpu.get_barrier_semaphore()
    for peer in (at_x(along_x(X - 1)), at_x(along_x(1)), at_y(along_y(Y - 1))):
        pl.semaphore_signal(barrier, inc=1, device_id=peer, device_id_type=MESH)

    first, rest = piece(0, LEAD), piece(LEAD, PIECES - LEAD)
    loads = [
        pltpu.make_async_copy(sig.at[:, first], mine.at[:, first], load_sem.at[0]),
        pltpu.make_async_copy(sig.at[:, rest], mine.at[:, rest], load_sem.at[1]),
        pltpu.make_async_copy(sig.at[x], row.at[x], load_sem.at[2]),
        pltpu.make_async_copy(gain_in, gain, load_sem.at[3]),
    ]
    for load in loads:
        load.start()
    acc[...] = jnp.zeros_like(acc)
    pl.semaphore_wait(barrier, 3)
    pl.semaphore_signal(ready, inc=1, device_id=at_x(along_x(X - 1)), device_id_type=MESH)

    def send_in(c, k):
        pltpu.make_async_remote_copy(
            src_ref=mine.at[c, piece(k)],
            dst_ref=row.at[x, piece(k)],
            send_sem=in_send,
            recv_sem=in_recv.at[k],
            device_id=at_x(c),
            device_id_type=MESH,
        ).start()

    def send_up(c, k):
        pltpu.make_async_remote_copy(
            src_ref=row.at[c, piece(k)],
            dst_ref=below.at[c - 1, piece(k)],
            send_sem=up_send,
            recv_sem=up_recv.at[k],
            device_id=at_y(along_y(1)),
            device_id_type=MESH,
        ).start()

    def send_out(d, k):
        c = along_x(d)
        pltpu.make_async_remote_copy(
            src_ref=mixed.at[c, piece(k)],
            dst_ref=back.at[x, piece(k)],
            send_sem=out_send,
            recv_sem=out_recv.at[k],
            device_id=at_x(c),
            device_id_type=MESH,
        ).start()

    def three(ref, k):
        return ref.at[: X - 1, piece(k)]

    loads[0].wait()
    for k in range(LEAD):
        send_in(along_x(1), k)
        send_in(along_x(3), k)
    pl.semaphore_wait(ready, 1)
    for k in range(LEAD):
        send_in(along_x(2), k)
    loads[1].wait()

    @pl.loop(LEAD, PIECES)
    def _(k):
        for c in (0, 2, 1, 3):

            @pl.when(x != c)
            def _(c=c):
                send_in(c, k)

    loads[2].wait()

    @pl.when(x > 0)
    def _():
        @pl.loop(0, PIECES)
        def _(k):
            send_up(x, k)

    loads[3].wait()

    def gather(k):
        wait_for(three(row, k), in_recv.at[k])
        for c in range(1, X):

            @pl.when(x != c)
            def _(c=c):
                send_up(c, k)

    def mix(k):
        wait_for(three(below, k), up_recv.at[k])
        g0, g1, g2 = (jnp.broadcast_to(gain[i : i + 1, :], (8, gain.shape[1])) for i in range(3))

        def block(i, total):
            rows = pl.ds(pl.multiple_of(k * R + i * BLOCK, BLOCK), BLOCK)
            taps = [below[c, rows, :] for c in range(X - 1)] + [row[c, rows, :] for c in range(X)]
            taps = [t.astype(jnp.float32).reshape(BLOCK // 8, 8, -1) for t in taps]
            for c in range(X):
                m = g0 * taps[c + 3] + g1 * taps[c + 1] + g2 * taps[c]
                total = total + jnp.sum(m * m, axis=0)
                mixed[c, rows, :] = m.reshape(BLOCK, -1).astype(jnp.bfloat16)
            return total

        acc[...] = lax.fori_loop(0, R // BLOCK, block, acc[...])

    def give_back(k):
        for d in (2, 1, 3):
            send_out(d, k)

    early = jnp.where(lax.rem(lax.axis_index("line"), 2) == 0, *EARLY)

    def early_back(k):
        @pl.when(k < early)
        def _():
            give_back(k)

    @pl.loop(0, LAG)
    def _(k):
        gather(k)

    @pl.loop(LAG, PIECES)
    def _(k):
        gather(k)
        mix(k - LAG)
        early_back(k - LAG)

    @pl.loop(PIECES - LAG, PIECES)
    def _(k):
        mix(k)
        early_back(k)

    for d in range(1, Y):
        pltpu.make_async_remote_copy(
            src_ref=acc, dst_ref=part_y.at[d - 1], send_sem=power_send.at[0], recv_sem=power_recv.at[0],
            device_id=at_y(along_y(d)), device_id_type=MESH,
        ).start()
    wait_for(part_y, power_recv.at[0])
    sum_y[...] = acc[...] + jnp.sum(part_y[...], axis=0)
    for d in range(1, X):
        pltpu.make_async_remote_copy(
            src_ref=sum_y, dst_ref=part_x.at[d - 1], send_sem=power_send.at[1], recv_sem=power_recv.at[1],
            device_id=at_x(along_x(d)), device_id_type=MESH,
        ).start()

    @pl.loop(0, PIECES)
    def _(k):
        @pl.when(k >= early)
        def _():
            give_back(k)

    wait_for(part_x, power_recv.at[1])
    total = sum_y[...] + jnp.sum(part_x[...], axis=0)
    power = jnp.sum(total, axis=0, keepdims=True) / (X * steps * phases)
    scale = jnp.broadcast_to(lax.rsqrt(power + 1e-05), (8, out.shape[2]))

    def finish(source, c, start, stop):
        @pl.loop(start // WIDE, stop // WIDE)
        def _(i):
            rows = pl.ds(pl.multiple_of(i * WIDE, WIDE), WIDE)
            m = source[c, rows, :].astype(jnp.float32).reshape(WIDE // 8, 8, -1) * scale
            out[c, rows, :] = m.reshape(WIDE, -1).astype(jnp.bfloat16)

    finish(mixed, x, 0, steps)

    @pl.loop(0, PIECES)
    def _(k):
        wait_for(three(back, k), out_recv.at[k])
        for d in range(1, X):
            finish(back, along_x(d), k * R, (k + 1) * R)

    wait_for(mine.at[: X - 1], in_send)
    wait_for(below, up_send)
    wait_for(mixed.at[: X - 1], out_send)
    wait_for(part_y, power_send.at[0])
    wait_for(part_x, power_send.at[1])


def body(signal, tap_gain):
    steps, channels = signal.shape[2:]
    Y = lax.axis_size("phase") // X
    part = steps // X
    dma = pltpu.SemaphoreType.DMA

    def rows(n):
        return pltpu.VMEM((n, part, channels), jnp.bfloat16)

    def sums(*n):
        return pltpu.VMEM((*n, 8, channels), jnp.float32)

    out = pl.pallas_call(
        kernel,
        name="echoes",
        out_shape=pltpu.VMEM((X, part, channels), signal.dtype),
        in_specs=[pl.BlockSpec(memory_space=pltpu.HBM)] * 2,
        out_specs=pl.BlockSpec(memory_space=pltpu.VMEM),
        scratch_shapes=[
            pltpu.VMEM(tap_gain.shape, jnp.float32),
            rows(X),
            rows(X),
            rows(X - 1),
            rows(X),
            rows(X),
            sums(),
            sums(X - 1),
            sums(Y - 1),
            sums(),
            pltpu.SemaphoreType.REGULAR,
            dma((4,)),
            dma(()),
            dma((PIECES,)),
            dma(()),
            dma((PIECES,)),
            dma(()),
            dma((PIECES,)),
            dma((2,)),
            dma((2,)),
        ],
        compiler_params=pltpu.CompilerParams(
            collective_id=0, has_side_effects=True, vmem_limit_bytes=VMEM
        ),
    )(signal.reshape(X, part, channels), tap_gain)
    return out.reshape(signal.shape)


def solution(mesh):
    return jax.shard_map(
        body,
        mesh=mesh,
        in_specs=(P("phase", "line", None, None), P()),
        out_specs=P("phase", "line", None, None),
        check_vma=False,
    )
```

```python
import jax
import jax.numpy as jnp
from jax import lax
from jax.experimental import pallas as pl
from jax.experimental.pallas import tpu as pltpu
from jax.sharding import PartitionSpec as P

MESH = pl.DeviceIdType.MESH
X = 4
PIECES = 8
LAG = 1
EARLY = 6
LEAD = 1
BLOCK = 16
WIDE = 64
MIB = 2**20
VMEM = 54 * MIB


def kernel(
    sig, gain_in, out, gain, mine, row, below, mixed, back, acc, part_x, part_y, sum_y,
    ready, load_sem, in_send, in_recv, up_send, up_recv, out_send, out_recv, power_send, power_recv,
):
    me = lax.axis_index("phase")
    phases = lax.axis_size("phase")
    Y = phases // X
    x, y = lax.rem(me, X), me // X
    steps = row.shape[1]
    R = steps // PIECES

    def along_x(d):
        return lax.rem(x + d, X)

    def along_y(d):
        return lax.rem(y + d, Y)

    def at_x(c):
        return {"phase": y * X + c}

    def at_y(r):
        return {"phase": r * X + x}

    def piece(k, count=1):
        return pl.ds(pl.multiple_of(k * R, R), count * R)

    def wait_for(ref, sem):
        pltpu.make_async_copy(ref, ref, sem).wait()

    barrier = pltpu.get_barrier_semaphore()
    for peer in (at_x(along_x(X - 1)), at_x(along_x(1)), at_y(along_y(Y - 1))):
        pl.semaphore_signal(barrier, inc=1, device_id=peer, device_id_type=MESH)

    first, rest = piece(0, LEAD), piece(LEAD, PIECES - LEAD)
    loads = [
        pltpu.make_async_copy(sig.at[:, first], mine.at[:, first], load_sem.at[0]),
        pltpu.make_async_copy(sig.at[:, rest], mine.at[:, rest], load_sem.at[1]),
        pltpu.make_async_copy(sig.at[x], row.at[x], load_sem.at[2]),
        pltpu.make_async_copy(gain_in, gain, load_sem.at[3]),
    ]
    for load in loads:
        load.start()
    acc[...] = jnp.zeros_like(acc)
    pl.semaphore_wait(barrier, 3)
    pl.semaphore_signal(ready, inc=1, device_id=at_x(along_x(X - 1)), device_id_type=MESH)

    def send_in(c, k):
        pltpu.make_async_remote_copy(
            src_ref=mine.at[c, piece(k)],
            dst_ref=row.at[x, piece(k)],
            send_sem=in_send,
            recv_sem=in_recv.at[k],
            device_id=at_x(c),
            device_id_type=MESH,
        ).start()

    def send_up(c, k):
        pltpu.make_async_remote_copy(
            src_ref=row.at[c, piece(k)],
            dst_ref=below.at[c - 1, piece(k)],
            send_sem=up_send,
            recv_sem=up_recv.at[k],
            device_id=at_y(along_y(1)),
            device_id_type=MESH,
        ).start()

    def send_out(d, k):
        c = along_x(d)
        pltpu.make_async_remote_copy(
            src_ref=mixed.at[c, piece(k)],
            dst_ref=back.at[x, piece(k)],
            send_sem=out_send,
            recv_sem=out_recv.at[k],
            device_id=at_x(c),
            device_id_type=MESH,
        ).start()

    def three(ref, k):
        return ref.at[: X - 1, piece(k)]

    loads[0].wait()
    for k in range(LEAD):
        send_in(along_x(1), k)
        send_in(along_x(3), k)
    pl.semaphore_wait(ready, 1)
    for k in range(LEAD):
        send_in(along_x(2), k)
    loads[1].wait()

    @pl.loop(LEAD, PIECES)
    def _(k):
        for c in (0, 2, 1, 3):

            @pl.when(x != c)
            def _(c=c):
                send_in(c, k)

    loads[2].wait()

    @pl.when(x > 0)
    def _():
        @pl.loop(0, PIECES)
        def _(k):
            send_up(x, k)

    loads[3].wait()

    def gather(k):
        wait_for(three(row, k), in_recv.at[k])
        for c in range(1, X):

            @pl.when(x != c)
            def _(c=c):
                send_up(c, k)

    def mix(k):
        wait_for(three(below, k), up_recv.at[k])
        g0, g1, g2 = (jnp.broadcast_to(gain[i : i + 1, :], (8, gain.shape[1])) for i in range(3))

        def block(i, total):
            rows = pl.ds(pl.multiple_of(k * R + i * BLOCK, BLOCK), BLOCK)
            taps = [below[c, rows, :] for c in range(X - 1)] + [row[c, rows, :] for c in range(X)]
            taps = [t.astype(jnp.float32).reshape(BLOCK // 8, 8, -1) for t in taps]
            for c in range(X):
                m = g0 * taps[c + 3] + g1 * taps[c + 1] + g2 * taps[c]
                total = total + jnp.sum(m * m, axis=0)
                mixed[c, rows, :] = m.reshape(BLOCK, -1).astype(jnp.bfloat16)
            return total

        acc[...] = lax.fori_loop(0, R // BLOCK, block, acc[...])

    def give_back(k):
        for d in (2, 1, 3):
            send_out(d, k)

    def stage(start, stop, *, first=True, second=True, third=True):
        if start < stop:

            @pl.loop(start, stop)
            def _(k):
                if first:
                    gather(k)
                if second:
                    mix(k - LAG)
                if second and third:
                    give_back(k - LAG)

    turn = min(EARLY + LAG, PIECES)
    stage(0, LAG, second=False)
    stage(LAG, turn)
    stage(turn, PIECES, third=False)
    stage(PIECES, EARLY + LAG, first=False)
    stage(max(PIECES, EARLY + LAG), PIECES + LAG, first=False, third=False)

    for d in range(1, Y):
        pltpu.make_async_remote_copy(
            src_ref=acc, dst_ref=part_y.at[d - 1], send_sem=power_send.at[0], recv_sem=power_recv.at[0],
            device_id=at_y(along_y(d)), device_id_type=MESH,
        ).start()
    wait_for(part_y, power_recv.at[0])
    sum_y[...] = acc[...] + jnp.sum(part_y[...], axis=0)
    for d in range(1, X):
        pltpu.make_async_remote_copy(
            src_ref=sum_y, dst_ref=part_x.at[d - 1], send_sem=power_send.at[1], recv_sem=power_recv.at[1],
            device_id=at_x(along_x(d)), device_id_type=MESH,
        ).start()

    @pl.loop(EARLY, PIECES)
    def _(k):
        give_back(k)

    wait_for(part_x, power_recv.at[1])
    total = sum_y[...] + jnp.sum(part_x[...], axis=0)
    power = jnp.sum(total, axis=0, keepdims=True) / (X * steps * phases)
    scale = jnp.broadcast_to(lax.rsqrt(power + 1e-05), (8, out.shape[2]))

    def finish(source, c, start, stop):
        @pl.loop(start // WIDE, stop // WIDE)
        def _(i):
            rows = pl.ds(pl.multiple_of(i * WIDE, WIDE), WIDE)
            m = source[c, rows, :].astype(jnp.float32).reshape(WIDE // 8, 8, -1) * scale
            out[c, rows, :] = m.reshape(WIDE, -1).astype(jnp.bfloat16)

    finish(mixed, x, 0, steps)

    @pl.loop(0, PIECES)
    def _(k):
        wait_for(three(back, k), out_recv.at[k])
        for d in range(1, X):
            finish(back, along_x(d), k * R, (k + 1) * R)

    wait_for(mine.at[: X - 1], in_send)
    wait_for(below, up_send)
    wait_for(mixed.at[: X - 1], out_send)
    wait_for(part_y, power_send.at[0])
    wait_for(part_x, power_send.at[1])


def body(signal, tap_gain):
    steps, channels = signal.shape[2:]
    Y = lax.axis_size("phase") // X
    part = steps // X
    dma = pltpu.SemaphoreType.DMA

    def rows(n):
        return pltpu.VMEM((n, part, channels), jnp.bfloat16)

    def sums(*n):
        return pltpu.VMEM((*n, 8, channels), jnp.float32)

    out = pl.pallas_call(
        kernel,
        name="echoes",
        out_shape=pltpu.VMEM((X, part, channels), signal.dtype),
        in_specs=[pl.BlockSpec(memory_space=pltpu.HBM)] * 2,
        out_specs=pl.BlockSpec(memory_space=pltpu.VMEM),
        scratch_shapes=[
            pltpu.VMEM(tap_gain.shape, jnp.float32),
            rows(X),
            rows(X),
            rows(X - 1),
            rows(X),
            rows(X),
            sums(),
            sums(X - 1),
            sums(Y - 1),
            sums(),
            pltpu.SemaphoreType.REGULAR,
            dma((4,)),
            dma(()),
            dma((PIECES,)),
            dma(()),
            dma((PIECES,)),
            dma(()),
            dma((PIECES,)),
            dma((2,)),
            dma((2,)),
        ],
        compiler_params=pltpu.CompilerParams(
            collective_id=0, has_side_effects=True, vmem_limit_bytes=VMEM
        ),
    )(signal.reshape(X, part, channels), tap_gain)
    return out.reshape(signal.shape)


def solution(mesh):
    return jax.shard_map(
        body,
        mesh=mesh,
        in_specs=(P("phase", "line", None, None), P()),
        out_specs=P("phase", "line", None, None),
        check_vma=False,
    )
```

```python
import functools

import jax
import jax.numpy as jnp
from jax import lax
from jax.experimental import pallas as pl
from jax.experimental.pallas import tpu as pltpu
from jax.sharding import PartitionSpec as P

MESH = pl.DeviceIdType.MESH
X = 4
ROWS = 192
LAG = 1
SHIFT = (-32, 32, 32, -32)
EARLY = 8
LEAD = 2
BLOCK = 16
WIDE = 96
MIB = 2**20
VMEM = 54 * MIB


def whole_pieces(even):
    return (even + min(SHIFT) - 1) // ROWS


def kernel(
    sig, gain_in, out, gain, mine, row, below, mixed, back, acc, part_x, part_y, sum_y,
    ready, load_sem, in_send, in_recv, up_send, up_recv, out_send, out_recv, power_send, power_recv,
):
    me = lax.axis_index("phase")
    phases = lax.axis_size("phase")
    Y = phases // X
    x, y = lax.rem(me, X), me // X
    even = out.shape[0] // X
    R, last = ROWS, whole_pieces(even)
    share = [even + SHIFT[c] for c in range(X)]
    begin = [sum(share[:c]) for c in range(X)]
    tail = [share[c] - last * R for c in range(X)]

    def along_x(d):
        return lax.rem(x + d, X)

    def along_y(d):
        return lax.rem(y + d, Y)

    def at_x(c):
        return {"phase": y * X + c}

    def at_y(r):
        return {"phase": r * X + x}

    def of(values, c):
        picked = jnp.int32(values[0])
        for i in range(1, X):
            picked = jnp.where(c == i, values[i], picked)
        return picked

    def by_column(values, work):
        for value in sorted(set(values)):
            here = [x == c for c in range(X) if values[c] == value]
            pl.when(functools.reduce(jnp.logical_or, here))(functools.partial(work, value))

    def rows(k, size=None):
        return pl.ds(pl.multiple_of(k * R, R), R if size is None else size)

    def wait_for(ref, sem):
        pltpu.make_async_copy(ref, ref, sem).wait()

    def load_own(size):
        start = pl.multiple_of(of(begin, x), 16)
        return pltpu.make_async_copy(sig.at[pl.ds(start, size)], row.at[x, :size], load_sem.at[2])

    barrier = pltpu.get_barrier_semaphore()
    for peer in (at_x(along_x(X - 1)), at_x(along_x(1)), at_y(along_y(Y - 1))):
        pl.semaphore_signal(barrier, inc=1, device_id=peer, device_id_type=MESH)

    loads = []
    for part in range(2):
        for c in range(X):
            start, stop = ((0, LEAD * R), (LEAD * R, share[c]))[part]
            piece = pl.ds(begin[c] + start, stop - start)
            loads.append(pltpu.make_async_copy(sig.at[piece], mine.at[piece], load_sem.at[part]))
    load_gain = pltpu.make_async_copy(gain_in, gain, load_sem.at[3])
    for load in loads:
        load.start()
    by_column(share, lambda size: load_own(size).start())
    load_gain.start()
    acc[...] = jnp.zeros_like(acc)
    pl.semaphore_wait(barrier, 3)
    pl.semaphore_signal(ready, inc=1, device_id=at_x(along_x(X - 1)), device_id_type=MESH)

    def send_in(c, k, size=None):
        start = pl.multiple_of((of(begin, c) if size is None else begin[c]) + k * R, 16)
        pltpu.make_async_remote_copy(
            src_ref=mine.at[pl.ds(start, R if size is None else size)],
            dst_ref=row.at[x, rows(k, size)],
            send_sem=in_send,
            recv_sem=in_recv.at[k],
            device_id=at_x(c),
            device_id_type=MESH,
        ).start()

    def send_up(c, k, size=None):
        pltpu.make_async_remote_copy(
            src_ref=row.at[c, rows(k, size)],
            dst_ref=below.at[c - 1, rows(k, size)],
            send_sem=up_send,
            recv_sem=up_recv.at[k],
            device_id=at_y(along_y(1)),
            device_id_type=MESH,
        ).start()

    def send_out(d, k, size=None):
        c = along_x(d)
        pltpu.make_async_remote_copy(
            src_ref=mixed.at[c, rows(k, size)],
            dst_ref=back.at[x, rows(k, size)],
            send_sem=out_send,
            recv_sem=out_recv.at[k],
            device_id=at_x(c),
            device_id_type=MESH,
        ).start()

    def three(ref, k, size=None):
        return ref.at[: X - 1, rows(k, size)]

    for load in loads[:X]:
        load.wait()
    for k in range(LEAD):
        send_in(along_x(1), k)
        send_in(along_x(3), k)
    pl.semaphore_wait(ready, 1)
    for k in range(LEAD):
        send_in(along_x(2), k)
    for load in loads[X:]:
        load.wait()

    def to_others(k, whole):
        for c in (0, 2, 1, 3):

            @pl.when(x != c)
            def _(c=c):
                send_in(c, k, R if whole else tail[c])

    @pl.loop(LEAD, last)
    def _(k):
        to_others(k, True)

    to_others(last, False)
    by_column(share, lambda size: load_own(size).wait())

    @pl.when(x > 0)
    def _():
        @pl.loop(0, last)
        def _(k):
            send_up(x, k)

        by_column(tail, lambda size: send_up(x, last, size))

    load_gain.wait()

    def gather(k, size=None):
        wait_for(three(row, k, size), in_recv.at[k])
        for c in range(1, X):

            @pl.when(x != c)
            def _(c=c):
                send_up(c, k, size)

    def mix(k, size=None):
        size = R if size is None else size
        wait_for(three(below, k, size), up_recv.at[k])
        g0, g1, g2 = (jnp.broadcast_to(gain[i : i + 1, :], (8, gain.shape[1])) for i in range(3))

        def block(i, total):
            at = pl.ds(pl.multiple_of(k * R + i * BLOCK, BLOCK), BLOCK)
            taps = [below[c, at, :] for c in range(X - 1)] + [row[c, at, :] for c in range(X)]
            taps = [t.astype(jnp.float32).reshape(BLOCK // 8, 8, -1) for t in taps]
            for c in range(X):
                m = g0 * taps[c + 3] + g1 * taps[c + 1] + g2 * taps[c]
                total = total + jnp.sum(m * m, axis=0)
                mixed[c, at, :] = m.reshape(BLOCK, -1).astype(jnp.bfloat16)
            return total

        acc[...] = lax.fori_loop(0, size // BLOCK, block, acc[...])

    def give_back(k, size=None):
        for d in (2, 1, 3):
            send_out(d, k, size)

    gather(0)

    @pl.loop(1, EARLY + 1)
    def _(k):
        gather(k)
        mix(k - 1)
        give_back(k - 1)

    @pl.loop(EARLY + 1, last)
    def _(k):
        gather(k)
        mix(k - 1)

    by_column(tail, lambda size: gather(last, size))
    mix(last - 1)
    by_column(tail, lambda size: mix(last, size))

    for d in range(1, Y):
        pltpu.make_async_remote_copy(
            src_ref=acc, dst_ref=part_y.at[d - 1], send_sem=power_send.at[0], recv_sem=power_recv.at[0],
            device_id=at_y(along_y(d)), device_id_type=MESH,
        ).start()
    wait_for(part_y, power_recv.at[0])
    sum_y[...] = acc[...] + jnp.sum(part_y[...], axis=0)
    for d in range(1, X):
        pltpu.make_async_remote_copy(
            src_ref=sum_y, dst_ref=part_x.at[d - 1], send_sem=power_send.at[1], recv_sem=power_recv.at[1],
            device_id=at_x(along_x(d)), device_id_type=MESH,
        ).start()

    @pl.loop(EARLY, last)
    def _(k):
        give_back(k)

    by_column(tail, lambda size: give_back(last, size))

    wait_for(part_x, power_recv.at[1])
    total = sum_y[...] + jnp.sum(part_x[...], axis=0)
    power = jnp.sum(total, axis=0, keepdims=True) / (X * even * phases)
    scale = jnp.broadcast_to(lax.rsqrt(power + 1e-05), (8, out.shape[1]))

    def finish(source, c, begins, start, size):
        m = source[c, pl.ds(start, size), :].astype(jnp.float32).reshape(size // 8, 8, -1) * scale
        at = pl.ds(pl.multiple_of(begins + start, 16), size)
        out[at, :] = m.reshape(size, -1).astype(jnp.bfloat16)

    def finish_piece(source, c, k):
        begins = of(begin, c)

        @pl.loop(0, R // WIDE)
        def _(i):
            finish(source, c, begins, pl.multiple_of(k * R + i * WIDE, 16), WIDE)

    @pl.loop(0, last)
    def _(k):
        finish_piece(mixed, x, k)

    by_column(tail, lambda size: finish(mixed, x, of(begin, x), last * R, size))

    @pl.loop(0, last)
    def _(k):
        wait_for(three(back, k), out_recv.at[k])
        for d in range(1, X):
            finish_piece(back, along_x(d), k)

    by_column([sum(tail) - t for t in tail], lambda n: wait_for(mine.at[:n], out_recv.at[last]))
    for c in range(X):

        @pl.when(x != c)
        def _(c=c):
            finish(back, c, begin[c], last * R, tail[c])

    by_column([sum(share) - t for t in share], lambda n: wait_for(mine.at[:n], in_send))
    by_column(share, lambda size: wait_for(below.at[:, :size], up_send))
    by_column(share, lambda size: wait_for(below.at[:, :size], out_send))
    wait_for(part_y, power_send.at[0])
    wait_for(part_x, power_send.at[1])


def body(signal, tap_gain):
    steps, channels = signal.shape[2:]
    Y = lax.axis_size("phase") // X
    part = steps // X + max(SHIFT)
    pieces = whole_pieces(steps // X) + 1
    dma = pltpu.SemaphoreType.DMA

    def rows(n):
        return pltpu.VMEM((n, part, channels), jnp.bfloat16)

    def sums(*n):
        return pltpu.VMEM((*n, 8, channels), jnp.float32)

    out = pl.pallas_call(
        kernel,
        name="echoes",
        out_shape=pltpu.VMEM((steps, channels), signal.dtype),
        in_specs=[pl.BlockSpec(memory_space=pltpu.HBM)] * 2,
        out_specs=pl.BlockSpec(memory_space=pltpu.VMEM),
        scratch_shapes=[
            pltpu.VMEM(tap_gain.shape, jnp.float32),
            pltpu.VMEM((steps, channels), jnp.bfloat16),
            rows(X),
            rows(X - 1),
            rows(X),
            rows(X),
            sums(),
            sums(X - 1),
            sums(Y - 1),
            sums(),
            pltpu.SemaphoreType.REGULAR,
            dma((4,)),
            dma(()),
            dma((pieces,)),
            dma(()),
            dma((pieces,)),
            dma(()),
            dma((pieces,)),
            dma((2,)),
            dma((2,)),
        ],
        compiler_params=pltpu.CompilerParams(
            collective_id=0, has_side_effects=True, vmem_limit_bytes=VMEM
        ),
    )(signal.reshape(steps, channels), tap_gain)
    return out.reshape(signal.shape)


def solution(mesh):
    return jax.shard_map(
        body,
        mesh=mesh,
        in_specs=(P("phase", "line", None, None), P()),
        out_specs=P("phase", "line", None, None),
        check_vma=False,
    )
```

```python
import functools

import jax
import jax.numpy as jnp
from jax import lax
from jax.experimental import pallas as pl
from jax.experimental.pallas import tpu as pltpu
from jax.sharding import PartitionSpec as P

MESH = pl.DeviceIdType.MESH
X = 4
ROWS = 192
LAG = 1
SHIFT = (-32, 48, 16, -32)
EARLY = 8
LEAD = 2
BLOCK = 16
WIDE = 96
MIB = 2**20
VMEM = 54 * MIB


def whole_pieces(even):
    return (even + min(SHIFT) - 1) // ROWS


def kernel(
    sig, gain_in, out, gain, mine, row, below, mixed, back, acc, part_x, part_y, sum_y,
    ready, load_sem, in_send, in_recv, up_send, up_recv, out_send, out_recv, power_send, power_recv,
):
    me = lax.axis_index("phase")
    phases = lax.axis_size("phase")
    Y = phases // X
    x, y = lax.rem(me, X), me // X
    even = out.shape[0] // X
    R, last = ROWS, whole_pieces(even)
    share = [even + SHIFT[c] for c in range(X)]
    begin = [sum(share[:c]) for c in range(X)]
    tail = [share[c] - last * R for c in range(X)]

    def along_x(d):
        return lax.rem(x + d, X)

    def along_y(d):
        return lax.rem(y + d, Y)

    def at_x(c):
        return {"phase": y * X + c}

    def at_y(r):
        return {"phase": r * X + x}

    def of(values, c):
        picked = jnp.int32(values[0])
        for i in range(1, X):
            picked = jnp.where(c == i, values[i], picked)
        return picked

    def by_column(values, work):
        for value in sorted(set(values)):
            here = [x == c for c in range(X) if values[c] == value]
            pl.when(functools.reduce(jnp.logical_or, here))(functools.partial(work, value))

    def rows(k, size=None):
        return pl.ds(pl.multiple_of(k * R, R), R if size is None else size)

    def wait_for(ref, sem):
        pltpu.make_async_copy(ref, ref, sem).wait()

    def load_own(size):
        start = pl.multiple_of(of(begin, x), 16)
        return pltpu.make_async_copy(sig.at[pl.ds(start, size)], row.at[x, :size], load_sem.at[2])

    barrier = pltpu.get_barrier_semaphore()

    def meet(condition, peer):
        @pl.when(condition)
        def _():
            pl.semaphore_signal(barrier, inc=1, device_id=peer, device_id_type=MESH)

    for c in range(1, X):
        meet(c > x, at_x(c))
    meet(y < Y - 1, at_y(along_y(1)))
    meet(y == 0, at_y(along_y(Y - 1)))

    loads = []
    for part in range(2):
        for c in range(X):
            start, stop = ((0, LEAD * R), (LEAD * R, share[c]))[part]
            piece = pl.ds(begin[c] + start, stop - start)
            loads.append(pltpu.make_async_copy(sig.at[piece], mine.at[piece], load_sem.at[part]))
    load_gain = pltpu.make_async_copy(gain_in, gain, load_sem.at[3])
    for load in loads:
        load.start()
    by_column(share, lambda size: load_own(size).start())
    load_gain.start()
    acc[...] = jnp.zeros_like(acc)
    met = x + jnp.where(y > 0, 1, 0) + jnp.where(y == Y - 1, 1, 0)

    @pl.when(met > 0)
    def _():
        pl.semaphore_wait(barrier, met)

    for c in range(X - 1):

        @pl.when(c < x)
        def _(c=c):
            pl.semaphore_signal(ready.at[x], inc=1, device_id=at_x(c), device_id_type=MESH)

    @pl.when(y > 0)
    def _():
        pl.semaphore_signal(ready.at[0], inc=1, device_id=at_y(along_y(Y - 1)), device_id_type=MESH)

    def send_in(c, k, size=None):
        start = pl.multiple_of((of(begin, c) if size is None else begin[c]) + k * R, 16)
        pltpu.make_async_remote_copy(
            src_ref=mine.at[pl.ds(start, R if size is None else size)],
            dst_ref=row.at[x, rows(k, size)],
            send_sem=in_send,
            recv_sem=in_recv.at[k],
            device_id=at_x(c),
            device_id_type=MESH,
        ).start()

    def send_up(c, k, size=None):
        pltpu.make_async_remote_copy(
            src_ref=row.at[c, rows(k, size)],
            dst_ref=below.at[c - 1, rows(k, size)],
            send_sem=up_send,
            recv_sem=up_recv.at[k],
            device_id=at_y(along_y(1)),
            device_id_type=MESH,
        ).start()

    def send_out(d, k, size=None):
        c = along_x(d)
        pltpu.make_async_remote_copy(
            src_ref=mixed.at[c, rows(k, size)],
            dst_ref=back.at[x, rows(k, size)],
            send_sem=out_send,
            recv_sem=out_recv.at[k],
            device_id=at_x(c),
            device_id_type=MESH,
        ).start()

    def three(ref, k, size=None):
        return ref.at[: X - 1, rows(k, size)]

    for load in loads[:X]:
        load.wait()
    for c in range(X - 1):
        for k in range(LEAD):

            @pl.when(c < x)
            def _(c=c, k=k):
                send_in(c, k)

    for c in range(1, X):

        @pl.when(c > x)
        def _(c=c):
            pl.semaphore_wait(ready.at[c], 1)
            for k in range(LEAD):
                send_in(c, k)

    for load in loads[X:]:
        load.wait()

    def to_others(k, whole):
        for c in (0, 2, 1, 3):

            @pl.when(x != c)
            def _(c=c):
                send_in(c, k, R if whole else tail[c])

    @pl.loop(LEAD, last)
    def _(k):
        to_others(k, True)

    to_others(last, False)
    by_column(share, lambda size: load_own(size).wait())

    @pl.when(y < Y - 1)
    def _():
        pl.semaphore_wait(ready.at[0], 1)

    @pl.when(x > 0)
    def _():
        @pl.loop(0, last)
        def _(k):
            send_up(x, k)

        by_column(tail, lambda size: send_up(x, last, size))

    load_gain.wait()

    def gather(k, size=None):
        wait_for(three(row, k, size), in_recv.at[k])
        for c in range(1, X):

            @pl.when(x != c)
            def _(c=c):
                send_up(c, k, size)

    def mix(k, size=None):
        size = R if size is None else size
        wait_for(three(below, k, size), up_recv.at[k])
        g0, g1, g2 = (jnp.broadcast_to(gain[i : i + 1, :], (8, gain.shape[1])) for i in range(3))

        def block(i, total):
            at = pl.ds(pl.multiple_of(k * R + i * BLOCK, BLOCK), BLOCK)
            taps = [below[c, at, :] for c in range(X - 1)] + [row[c, at, :] for c in range(X)]
            taps = [t.astype(jnp.float32).reshape(BLOCK // 8, 8, -1) for t in taps]
            for c in range(X):
                m = g0 * taps[c + 3] + g1 * taps[c + 1] + g2 * taps[c]
                total = total + jnp.sum(m * m, axis=0)
                mixed[c, at, :] = m.reshape(BLOCK, -1).astype(jnp.bfloat16)
            return total

        acc[...] = lax.fori_loop(0, size // BLOCK, block, acc[...])

    def give_back(k, size=None):
        for d in (2, 1, 3):
            send_out(d, k, size)

    gather(0)

    @pl.loop(1, EARLY + 1)
    def _(k):
        gather(k)
        mix(k - 1)
        give_back(k - 1)

    @pl.loop(EARLY + 1, last)
    def _(k):
        gather(k)
        mix(k - 1)

    by_column(tail, lambda size: gather(last, size))
    mix(last - 1)
    by_column(tail, lambda size: mix(last, size))

    for d in range(1, Y):
        pltpu.make_async_remote_copy(
            src_ref=acc, dst_ref=part_y.at[d - 1], send_sem=power_send.at[0], recv_sem=power_recv.at[0],
            device_id=at_y(along_y(d)), device_id_type=MESH,
        ).start()
    wait_for(part_y, power_recv.at[0])
    sum_y[...] = acc[...] + jnp.sum(part_y[...], axis=0)
    for d in range(1, X):
        pltpu.make_async_remote_copy(
            src_ref=sum_y, dst_ref=part_x.at[d - 1], send_sem=power_send.at[1], recv_sem=power_recv.at[1],
            device_id=at_x(along_x(d)), device_id_type=MESH,
        ).start()

    @pl.loop(EARLY, last)
    def _(k):
        give_back(k)

    by_column(tail, lambda size: give_back(last, size))

    wait_for(part_x, power_recv.at[1])
    total = sum_y[...] + jnp.sum(part_x[...], axis=0)
    power = jnp.sum(total, axis=0, keepdims=True) / (X * even * phases)
    scale = jnp.broadcast_to(lax.rsqrt(power + 1e-05), (8, out.shape[1]))

    def finish(source, c, begins, start, size):
        m = source[c, pl.ds(start, size), :].astype(jnp.float32).reshape(size // 8, 8, -1) * scale
        at = pl.ds(pl.multiple_of(begins + start, 16), size)
        out[at, :] = m.reshape(size, -1).astype(jnp.bfloat16)

    def finish_piece(source, c, k):
        begins = of(begin, c)

        @pl.loop(0, R // WIDE)
        def _(i):
            finish(source, c, begins, pl.multiple_of(k * R + i * WIDE, 16), WIDE)

    @pl.loop(0, last)
    def _(k):
        finish_piece(mixed, x, k)

    by_column(tail, lambda size: finish(mixed, x, of(begin, x), last * R, size))

    @pl.loop(0, last)
    def _(k):
        wait_for(three(back, k), out_recv.at[k])
        for d in range(1, X):
            finish_piece(back, along_x(d), k)

    by_column([sum(tail) - t for t in tail], lambda n: wait_for(mine.at[:n], out_recv.at[last]))
    for c in range(X):

        @pl.when(x != c)
        def _(c=c):
            finish(back, c, begin[c], last * R, tail[c])

    by_column([sum(share) - t for t in share], lambda n: wait_for(mine.at[:n], in_send))
    by_column(share, lambda size: wait_for(below.at[:, :size], up_send))
    by_column(share, lambda size: wait_for(below.at[:, :size], out_send))
    wait_for(part_y, power_send.at[0])
    wait_for(part_x, power_send.at[1])


def body(signal, tap_gain):
    steps, channels = signal.shape[2:]
    Y = lax.axis_size("phase") // X
    part = steps // X + max(SHIFT)
    pieces = whole_pieces(steps // X) + 1
    dma = pltpu.SemaphoreType.DMA

    def rows(n):
        return pltpu.VMEM((n, part, channels), jnp.bfloat16)

    def sums(*n):
        return pltpu.VMEM((*n, 8, channels), jnp.float32)

    out = pl.pallas_call(
        kernel,
        name="echoes",
        out_shape=pltpu.VMEM((steps, channels), signal.dtype),
        in_specs=[pl.BlockSpec(memory_space=pltpu.HBM)] * 2,
        out_specs=pl.BlockSpec(memory_space=pltpu.VMEM),
        scratch_shapes=[
            pltpu.VMEM(tap_gain.shape, jnp.float32),
            pltpu.VMEM((steps, channels), jnp.bfloat16),
            rows(X),
            rows(X - 1),
            rows(X),
            rows(X),
            sums(),
            sums(X - 1),
            sums(Y - 1),
            sums(),
            pltpu.SemaphoreType.REGULAR((X,)),
            dma((4,)),
            dma(()),
            dma((pieces,)),
            dma(()),
            dma((pieces,)),
            dma(()),
            dma((pieces,)),
            dma((2,)),
            dma((2,)),
        ],
        compiler_params=pltpu.CompilerParams(
            collective_id=0, has_side_effects=True, vmem_limit_bytes=VMEM
        ),
    )(signal.reshape(steps, channels), tap_gain)
    return out.reshape(signal.shape)


def solution(mesh):
    return jax.shard_map(
        body,
        mesh=mesh,
        in_specs=(P("phase", "line", None, None), P()),
        out_specs=P("phase", "line", None, None),
        check_vma=False,
    )
```

```python
import functools

import jax
import jax.numpy as jnp
from jax import lax
from jax.experimental import pallas as pl
from jax.experimental.pallas import tpu as pltpu
from jax.sharding import PartitionSpec as P

MESH = pl.DeviceIdType.MESH
X = 4
ROWS = 192
LAG = 1
SHIFT = (-32, 48, 16, -32)
EARLY = 9
LEAD = 2
BLOCK = 16
WIDE = 96
MIB = 2**20
VMEM = 54 * MIB


def whole_pieces(even):
    return (even + min(SHIFT) - 1) // ROWS


def kernel(
    sig, gain_in, out, gain, mine, row, below, mixed, back, acc, part_x, part_y, sum_y,
    ready, load_sem, in_send, in_recv, up_send, up_recv, out_send, out_recv, power_send, power_recv,
):
    me = lax.axis_index("phase")
    phases = lax.axis_size("phase")
    Y = phases // X
    x, y = lax.rem(me, X), me // X
    even = out.shape[0] // X
    R, last = ROWS, whole_pieces(even)
    share = [even + SHIFT[c] for c in range(X)]
    begin = [sum(share[:c]) for c in range(X)]
    tail = [share[c] - last * R for c in range(X)]

    def along_x(d):
        return lax.rem(x + d, X)

    def along_y(d):
        return lax.rem(y + d, Y)

    def at_x(c):
        return {"phase": y * X + c}

    def at_y(r):
        return {"phase": r * X + x}

    def of(values, c):
        picked = jnp.int32(values[0])
        for i in range(1, X):
            picked = jnp.where(c == i, values[i], picked)
        return picked

    def by_column(values, work):
        for value in sorted(set(values)):
            here = [x == c for c in range(X) if values[c] == value]
            pl.when(functools.reduce(jnp.logical_or, here))(functools.partial(work, value))

    def rows(k, size=None):
        return pl.ds(pl.multiple_of(k * R, R), R if size is None else size)

    def wait_for(ref, sem):
        pltpu.make_async_copy(ref, ref, sem).wait()

    def load_own(size):
        start = pl.multiple_of(of(begin, x), 16)
        return pltpu.make_async_copy(sig.at[pl.ds(start, size)], row.at[x, :size], load_sem.at[2])

    barrier = pltpu.get_barrier_semaphore()

    def meet(condition, peer):
        @pl.when(condition)
        def _():
            pl.semaphore_signal(barrier, inc=1, device_id=peer, device_id_type=MESH)

    for c in range(1, X):
        meet(c > x, at_x(c))
    meet(y < Y - 1, at_y(along_y(1)))
    meet(y == 0, at_y(along_y(Y - 1)))

    loads = []
    for part in range(2):
        for c in range(X):
            start, stop = ((0, LEAD * R), (LEAD * R, share[c]))[part]
            piece = pl.ds(begin[c] + start, stop - start)
            loads.append(pltpu.make_async_copy(sig.at[piece], mine.at[piece], load_sem.at[part]))
    load_gain = pltpu.make_async_copy(gain_in, gain, load_sem.at[3])
    for load in loads:
        load.start()
    by_column(share, lambda size: load_own(size).start())
    load_gain.start()
    acc[...] = jnp.zeros_like(acc)
    met = x + jnp.where(y > 0, 1, 0) + jnp.where(y == Y - 1, 1, 0)

    @pl.when(met > 0)
    def _():
        pl.semaphore_wait(barrier, met)

    for c in range(X - 1):

        @pl.when(c < x)
        def _(c=c):
            pl.semaphore_signal(ready.at[x], inc=1, device_id=at_x(c), device_id_type=MESH)

    @pl.when(y > 0)
    def _():
        pl.semaphore_signal(ready.at[0], inc=1, device_id=at_y(along_y(Y - 1)), device_id_type=MESH)

    def send_in(c, k, size=None):
        start = pl.multiple_of((of(begin, c) if size is None else begin[c]) + k * R, 16)
        pltpu.make_async_remote_copy(
            src_ref=mine.at[pl.ds(start, R if size is None else size)],
            dst_ref=row.at[x, rows(k, size)],
            send_sem=in_send,
            recv_sem=in_recv.at[k],
            device_id=at_x(c),
            device_id_type=MESH,
        ).start()

    def send_up(c, k, size=None):
        pltpu.make_async_remote_copy(
            src_ref=row.at[c, rows(k, size)],
            dst_ref=below.at[c - 1, rows(k, size)],
            send_sem=up_send,
            recv_sem=up_recv.at[k],
            device_id=at_y(along_y(1)),
            device_id_type=MESH,
        ).start()

    def send_out(d, k, size=None):
        c = along_x(d)
        pltpu.make_async_remote_copy(
            src_ref=mixed.at[c, rows(k, size)],
            dst_ref=back.at[x, rows(k, size)],
            send_sem=out_send,
            recv_sem=out_recv.at[k],
            device_id=at_x(c),
            device_id_type=MESH,
        ).start()

    def three(ref, k, size=None):
        return ref.at[: X - 1, rows(k, size)]

    for load in loads[:X]:
        load.wait()
    for c in range(X - 1):
        for k in range(LEAD):

            @pl.when(c < x)
            def _(c=c, k=k):
                send_in(c, k)

    for c in range(1, X):

        @pl.when(c > x)
        def _(c=c):
            pl.semaphore_wait(ready.at[c], 1)
            for k in range(LEAD):
                send_in(c, k)

    for load in loads[X:]:
        load.wait()

    def to_others(k, whole):
        for c in (0, 2, 1, 3):

            @pl.when(x != c)
            def _(c=c):
                send_in(c, k, R if whole else tail[c])

    @pl.loop(LEAD, last)
    def _(k):
        to_others(k, True)

    to_others(last, False)
    by_column(share, lambda size: load_own(size).wait())

    @pl.when(y < Y - 1)
    def _():
        pl.semaphore_wait(ready.at[0], 1)

    @pl.when(x > 0)
    def _():
        @pl.loop(0, last)
        def _(k):
            send_up(x, k)

        by_column(tail, lambda size: send_up(x, last, size))

    load_gain.wait()

    def gather(k, size=None):
        wait_for(three(row, k, size), in_recv.at[k])
        for c in range(1, X):

            @pl.when(x != c)
            def _(c=c):
                send_up(c, k, size)

    def mix(k, size=None):
        size = R if size is None else size
        wait_for(three(below, k, size), up_recv.at[k])
        g0, g1, g2 = (jnp.broadcast_to(gain[i : i + 1, :], (8, gain.shape[1])) for i in range(3))

        def block(i, total):
            at = pl.ds(pl.multiple_of(k * R + i * BLOCK, BLOCK), BLOCK)
            taps = [below[c, at, :] for c in range(X - 1)] + [row[c, at, :] for c in range(X)]
            taps = [t.astype(jnp.float32).reshape(BLOCK // 8, 8, -1) for t in taps]
            for c in range(X):
                m = g0 * taps[c + 3] + g1 * taps[c + 1] + g2 * taps[c]
                total = total + jnp.sum(m * m, axis=0)
                mixed[c, at, :] = m.reshape(BLOCK, -1).astype(jnp.bfloat16)
            return total

        acc[...] = lax.fori_loop(0, size // BLOCK, block, acc[...])

    def give_back(k, size=None):
        for d in (2, 1, 3):
            send_out(d, k, size)

    gather(0)

    @pl.loop(1, EARLY + 1)
    def _(k):
        gather(k)
        mix(k - 1)
        give_back(k - 1)

    @pl.loop(EARLY + 1, last)
    def _(k):
        gather(k)
        mix(k - 1)

    by_column(tail, lambda size: gather(last, size))
    mix(last - 1)
    by_column(tail, lambda size: mix(last, size))

    for d in range(1, Y):
        pltpu.make_async_remote_copy(
            src_ref=acc, dst_ref=part_y.at[d - 1], send_sem=power_send.at[0], recv_sem=power_recv.at[0],
            device_id=at_y(along_y(d)), device_id_type=MESH,
        ).start()
    wait_for(part_y, power_recv.at[0])
    sum_y[...] = acc[...] + jnp.sum(part_y[...], axis=0)
    for d in range(1, X):
        pltpu.make_async_remote_copy(
            src_ref=sum_y, dst_ref=part_x.at[d - 1], send_sem=power_send.at[1], recv_sem=power_recv.at[1],
            device_id=at_x(along_x(d)), device_id_type=MESH,
        ).start()

    @pl.loop(EARLY, last)
    def _(k):
        give_back(k)

    by_column(tail, lambda size: give_back(last, size))

    wait_for(part_x, power_recv.at[1])
    total = sum_y[...] + jnp.sum(part_x[...], axis=0)
    power = jnp.sum(total, axis=0, keepdims=True) / (X * even * phases)
    scale = jnp.broadcast_to(lax.rsqrt(power + 1e-05), (8, out.shape[1]))

    def finish(source, c, begins, start, size):
        m = source[c, pl.ds(start, size), :].astype(jnp.float32).reshape(size // 8, 8, -1) * scale
        at = pl.ds(pl.multiple_of(begins + start, 16), size)
        out[at, :] = m.reshape(size, -1).astype(jnp.bfloat16)

    def finish_piece(source, c, k):
        begins = of(begin, c)

        @pl.loop(0, R // WIDE)
        def _(i):
            finish(source, c, begins, pl.multiple_of(k * R + i * WIDE, 16), WIDE)

    @pl.loop(0, last)
    def _(k):
        finish_piece(mixed, x, k)

    by_column(tail, lambda size: finish(mixed, x, of(begin, x), last * R, size))

    @pl.loop(0, last)
    def _(k):
        wait_for(three(back, k), out_recv.at[k])
        for d in range(1, X):
            finish_piece(back, along_x(d), k)

    by_column([sum(tail) - t for t in tail], lambda n: wait_for(mine.at[:n], out_recv.at[last]))
    for c in range(X):

        @pl.when(x != c)
        def _(c=c):
            finish(back, c, begin[c], last * R, tail[c])

    by_column([sum(share) - t for t in share], lambda n: wait_for(mine.at[:n], in_send))
    by_column(share, lambda size: wait_for(below.at[:, :size], up_send))
    by_column(share, lambda size: wait_for(below.at[:, :size], out_send))
    wait_for(part_y, power_send.at[0])
    wait_for(part_x, power_send.at[1])


def body(signal, tap_gain):
    steps, channels = signal.shape[2:]
    Y = lax.axis_size("phase") // X
    part = steps // X + max(SHIFT)
    pieces = whole_pieces(steps // X) + 1
    dma = pltpu.SemaphoreType.DMA

    def rows(n):
        return pltpu.VMEM((n, part, channels), jnp.bfloat16)

    def sums(*n):
        return pltpu.VMEM((*n, 8, channels), jnp.float32)

    out = pl.pallas_call(
        kernel,
        name="echoes",
        out_shape=pltpu.VMEM((steps, channels), signal.dtype),
        in_specs=[pl.BlockSpec(memory_space=pltpu.HBM)] * 2,
        out_specs=pl.BlockSpec(memory_space=pltpu.VMEM),
        scratch_shapes=[
            pltpu.VMEM(tap_gain.shape, jnp.float32),
            pltpu.VMEM((steps, channels), jnp.bfloat16),
            rows(X),
            rows(X - 1),
            rows(X),
            rows(X),
            sums(),
            sums(X - 1),
            sums(Y - 1),
            sums(),
            pltpu.SemaphoreType.REGULAR((X,)),
            dma((4,)),
            dma(()),
            dma((pieces,)),
            dma(()),
            dma((pieces,)),
            dma(()),
            dma((pieces,)),
            dma((2,)),
            dma((2,)),
        ],
        compiler_params=pltpu.CompilerParams(
            collective_id=0, has_side_effects=True, vmem_limit_bytes=VMEM
        ),
    )(signal.reshape(steps, channels), tap_gain)
    return out.reshape(signal.shape)


def solution(mesh):
    return jax.shard_map(
        body,
        mesh=mesh,
        in_specs=(P("phase", "line", None, None), P()),
        out_specs=P("phase", "line", None, None),
        check_vma=False,
    )
```

```python
import functools

import jax
import jax.numpy as jnp
from jax import lax
from jax.experimental import pallas as pl
from jax.experimental.pallas import tpu as pltpu
from jax.sharding import PartitionSpec as P

MESH = pl.DeviceIdType.MESH
X = 4
ROWS = 192
LAG = 1
SHIFT = (-32, 32, 48, -48)
EARLY = 9
LEAD = 2
BLOCK = 16
WIDE = 96
MIB = 2**20
VMEM = 54 * MIB


def whole_pieces(even):
    return (even + min(SHIFT) - 1) // ROWS


def kernel(
    sig, gain_in, out, gain, mine, row, below, mixed, back, acc, part_x, part_y, sum_y,
    ready, load_sem, in_send, in_recv, up_send, up_recv, out_send, out_recv, power_send, power_recv,
):
    me = lax.axis_index("phase")
    phases = lax.axis_size("phase")
    Y = phases // X
    x, y = lax.rem(me, X), me // X
    even = out.shape[0] // X
    R, last = ROWS, whole_pieces(even)
    share = [even + SHIFT[c] for c in range(X)]
    begin = [sum(share[:c]) for c in range(X)]
    tail = [share[c] - last * R for c in range(X)]

    def along_x(d):
        return lax.rem(x + d, X)

    def along_y(d):
        return lax.rem(y + d, Y)

    def at_x(c):
        return {"phase": y * X + c}

    def at_y(r):
        return {"phase": r * X + x}

    def of(values, c):
        picked = jnp.int32(values[0])
        for i in range(1, X):
            picked = jnp.where(c == i, values[i], picked)
        return picked

    def by_column(values, work):
        for value in sorted(set(values)):
            here = [x == c for c in range(X) if values[c] == value]
            pl.when(functools.reduce(jnp.logical_or, here))(functools.partial(work, value))

    def rows(k, size=None):
        return pl.ds(pl.multiple_of(k * R, R), R if size is None else size)

    def wait_for(ref, sem):
        pltpu.make_async_copy(ref, ref, sem).wait()

    def load_own(size):
        start = pl.multiple_of(of(begin, x), 16)
        return pltpu.make_async_copy(sig.at[pl.ds(start, size)], row.at[x, :size], load_sem.at[2])

    barrier = pltpu.get_barrier_semaphore()

    def meet(condition, peer):
        @pl.when(condition)
        def _():
            pl.semaphore_signal(barrier, inc=1, device_id=peer, device_id_type=MESH)

    for c in range(1, X):
        meet(c > x, at_x(c))
    meet(y < Y - 1, at_y(along_y(1)))
    meet(y == 0, at_y(along_y(Y - 1)))

    loads = []
    for part in range(2):
        for c in range(X):
            start, stop = ((0, LEAD * R), (LEAD * R, share[c]))[part]
            piece = pl.ds(begin[c] + start, stop - start)
            loads.append(pltpu.make_async_copy(sig.at[piece], mine.at[piece], load_sem.at[part]))
    load_gain = pltpu.make_async_copy(gain_in, gain, load_sem.at[3])
    for load in loads:
        load.start()
    by_column(share, lambda size: load_own(size).start())
    load_gain.start()
    acc[...] = jnp.zeros_like(acc)
    met = x + jnp.where(y > 0, 1, 0) + jnp.where(y == Y - 1, 1, 0)

    @pl.when(met > 0)
    def _():
        pl.semaphore_wait(barrier, met)

    for c in range(X - 1):

        @pl.when(c < x)
        def _(c=c):
            pl.semaphore_signal(ready.at[x], inc=1, device_id=at_x(c), device_id_type=MESH)

    @pl.when(y > 0)
    def _():
        pl.semaphore_signal(ready.at[0], inc=1, device_id=at_y(along_y(Y - 1)), device_id_type=MESH)

    def send_in(c, k, size=None):
        start = pl.multiple_of((of(begin, c) if size is None else begin[c]) + k * R, 16)
        pltpu.make_async_remote_copy(
            src_ref=mine.at[pl.ds(start, R if size is None else size)],
            dst_ref=row.at[x, rows(k, size)],
            send_sem=in_send,
            recv_sem=in_recv.at[k],
            device_id=at_x(c),
            device_id_type=MESH,
        ).start()

    def send_up(c, k, size=None):
        pltpu.make_async_remote_copy(
            src_ref=row.at[c, rows(k, size)],
            dst_ref=below.at[c - 1, rows(k, size)],
            send_sem=up_send,
            recv_sem=up_recv.at[k],
            device_id=at_y(along_y(1)),
            device_id_type=MESH,
        ).start()

    def send_out(d, k, size=None):
        c = along_x(d)
        pltpu.make_async_remote_copy(
            src_ref=mixed.at[c, rows(k, size)],
            dst_ref=back.at[x, rows(k, size)],
            send_sem=out_send,
            recv_sem=out_recv.at[k],
            device_id=at_x(c),
            device_id_type=MESH,
        ).start()

    def three(ref, k, size=None):
        return ref.at[: X - 1, rows(k, size)]

    for load in loads[:X]:
        load.wait()
    for c in range(X - 1):
        for k in range(LEAD):

            @pl.when(c < x)
            def _(c=c, k=k):
                send_in(c, k)

    for c in range(1, X):

        @pl.when(c > x)
        def _(c=c):
            pl.semaphore_wait(ready.at[c], 1)
            for k in range(LEAD):
                send_in(c, k)

    for load in loads[X:]:
        load.wait()

    def to_others(k, whole):
        for c in (0, 2, 1, 3):

            @pl.when(x != c)
            def _(c=c):
                send_in(c, k, R if whole else tail[c])

    @pl.loop(LEAD, last)
    def _(k):
        to_others(k, True)

    to_others(last, False)
    by_column(share, lambda size: load_own(size).wait())

    @pl.when(y < Y - 1)
    def _():
        pl.semaphore_wait(ready.at[0], 1)

    @pl.when(x > 0)
    def _():
        @pl.loop(0, last)
        def _(k):
            send_up(x, k)

        by_column(tail, lambda size: send_up(x, last, size))

    load_gain.wait()

    def gather(k, size=None):
        wait_for(three(row, k, size), in_recv.at[k])
        for c in range(1, X):

            @pl.when(x != c)
            def _(c=c):
                send_up(c, k, size)

    def mix(k, size=None):
        size = R if size is None else size
        wait_for(three(below, k, size), up_recv.at[k])
        g0, g1, g2 = (jnp.broadcast_to(gain[i : i + 1, :], (8, gain.shape[1])) for i in range(3))

        def block(i, total):
            at = pl.ds(pl.multiple_of(k * R + i * BLOCK, BLOCK), BLOCK)
            taps = [below[c, at, :] for c in range(X - 1)] + [row[c, at, :] for c in range(X)]
            taps = [t.astype(jnp.float32).reshape(BLOCK // 8, 8, -1) for t in taps]
            for c in range(X):
                m = g0 * taps[c + 3] + g1 * taps[c + 1] + g2 * taps[c]
                total = total + jnp.sum(m * m, axis=0)
                mixed[c, at, :] = m.reshape(BLOCK, -1).astype(jnp.bfloat16)
            return total

        acc[...] = lax.fori_loop(0, size // BLOCK, block, acc[...])

    def give_back(k, size=None):
        for d in (2, 1, 3):
            send_out(d, k, size)

    gather(0)

    @pl.loop(1, EARLY + 1)
    def _(k):
        gather(k)
        mix(k - 1)
        give_back(k - 1)

    @pl.loop(EARLY + 1, last)
    def _(k):
        gather(k)
        mix(k - 1)

    by_column(tail, lambda size: gather(last, size))
    mix(last - 1)
    by_column(tail, lambda size: mix(last, size))

    for d in range(1, Y):
        pltpu.make_async_remote_copy(
            src_ref=acc, dst_ref=part_y.at[d - 1], send_sem=power_send.at[0], recv_sem=power_recv.at[0],
            device_id=at_y(along_y(d)), device_id_type=MESH,
        ).start()
    wait_for(part_y, power_recv.at[0])
    sum_y[...] = acc[...] + jnp.sum(part_y[...], axis=0)
    for d in range(1, X):
        pltpu.make_async_remote_copy(
            src_ref=sum_y, dst_ref=part_x.at[d - 1], send_sem=power_send.at[1], recv_sem=power_recv.at[1],
            device_id=at_x(along_x(d)), device_id_type=MESH,
        ).start()

    @pl.loop(EARLY, last)
    def _(k):
        give_back(k)

    by_column(tail, lambda size: give_back(last, size))

    wait_for(part_x, power_recv.at[1])
    total = sum_y[...] + jnp.sum(part_x[...], axis=0)
    power = jnp.sum(total, axis=0, keepdims=True) / (X * even * phases)
    scale = jnp.broadcast_to(lax.rsqrt(power + 1e-05), (8, out.shape[1]))

    def finish(source, c, begins, start, size):
        m = source[c, pl.ds(start, size), :].astype(jnp.float32).reshape(size // 8, 8, -1) * scale
        at = pl.ds(pl.multiple_of(begins + start, 16), size)
        out[at, :] = m.reshape(size, -1).astype(jnp.bfloat16)

    def finish_piece(source, c, k):
        begins = of(begin, c)

        @pl.loop(0, R // WIDE)
        def _(i):
            finish(source, c, begins, pl.multiple_of(k * R + i * WIDE, 16), WIDE)

    @pl.loop(0, last)
    def _(k):
        finish_piece(mixed, x, k)

    by_column(tail, lambda size: finish(mixed, x, of(begin, x), last * R, size))

    @pl.loop(0, last)
    def _(k):
        wait_for(three(back, k), out_recv.at[k])
        for d in range(1, X):
            finish_piece(back, along_x(d), k)

    by_column([sum(tail) - t for t in tail], lambda n: wait_for(mine.at[:n], out_recv.at[last]))
    for c in range(X):

        @pl.when(x != c)
        def _(c=c):
            finish(back, c, begin[c], last * R, tail[c])

    by_column([sum(share) - t for t in share], lambda n: wait_for(mine.at[:n], in_send))
    by_column(share, lambda size: wait_for(below.at[:, :size], up_send))
    by_column(share, lambda size: wait_for(below.at[:, :size], out_send))
    wait_for(part_y, power_send.at[0])
    wait_for(part_x, power_send.at[1])


def body(signal, tap_gain):
    steps, channels = signal.shape[2:]
    Y = lax.axis_size("phase") // X
    part = steps // X + max(SHIFT)
    pieces = whole_pieces(steps // X) + 1
    dma = pltpu.SemaphoreType.DMA

    def rows(n):
        return pltpu.VMEM((n, part, channels), jnp.bfloat16)

    def sums(*n):
        return pltpu.VMEM((*n, 8, channels), jnp.float32)

    out = pl.pallas_call(
        kernel,
        name="echoes",
        out_shape=pltpu.VMEM((steps, channels), signal.dtype),
        in_specs=[pl.BlockSpec(memory_space=pltpu.HBM)] * 2,
        out_specs=pl.BlockSpec(memory_space=pltpu.VMEM),
        scratch_shapes=[
            pltpu.VMEM(tap_gain.shape, jnp.float32),
            pltpu.VMEM((steps, channels), jnp.bfloat16),
            rows(X),
            rows(X - 1),
            rows(X),
            rows(X),
            sums(),
            sums(X - 1),
            sums(Y - 1),
            sums(),
            pltpu.SemaphoreType.REGULAR((X,)),
            dma((4,)),
            dma(()),
            dma((pieces,)),
            dma(()),
            dma((pieces,)),
            dma(()),
            dma((pieces,)),
            dma((2,)),
            dma((2,)),
        ],
        compiler_params=pltpu.CompilerParams(
            collective_id=0, has_side_effects=True, vmem_limit_bytes=VMEM
        ),
    )(signal.reshape(steps, channels), tap_gain)
    return out.reshape(signal.shape)


def solution(mesh):
    return jax.shard_map(
        body,
        mesh=mesh,
        in_specs=(P("phase", "line", None, None), P()),
        out_specs=P("phase", "line", None, None),
        check_vma=False,
    )
```

```python
import functools

import jax
import jax.numpy as jnp
from jax import lax
from jax.experimental import pallas as pl
from jax.experimental.pallas import tpu as pltpu
from jax.sharding import PartitionSpec as P

MESH = pl.DeviceIdType.MESH
X = 4
ROWS = 240
LAG = 1
SHIFT = (-32, 32, 48, -48)
EARLY = 7
LEAD = 1
BLOCK = 16
WIDE = 80
MIB = 2**20
VMEM = 54 * MIB


def whole_pieces(even):
    return (even + min(SHIFT) - 1) // ROWS


def kernel(
    sig, gain_in, out, gain, mine, row, below, mixed, back, acc, part_x, part_y, sum_y,
    ready, load_sem, in_send, in_recv, up_send, up_recv, out_send, out_recv, power_send, power_recv,
):
    me = lax.axis_index("phase")
    phases = lax.axis_size("phase")
    Y = phases // X
    x, y = lax.rem(me, X), me // X
    even = out.shape[0] // X
    R, last = ROWS, whole_pieces(even)
    share = [even + SHIFT[c] for c in range(X)]
    begin = [sum(share[:c]) for c in range(X)]
    tail = [share[c] - last * R for c in range(X)]

    def along_x(d):
        return lax.rem(x + d, X)

    def along_y(d):
        return lax.rem(y + d, Y)

    def at_x(c):
        return {"phase": y * X + c}

    def at_y(r):
        return {"phase": r * X + x}

    def of(values, c):
        picked = jnp.int32(values[0])
        for i in range(1, X):
            picked = jnp.where(c == i, values[i], picked)
        return picked

    def by_column(values, work):
        for value in sorted(set(values)):
            here = [x == c for c in range(X) if values[c] == value]
            pl.when(functools.reduce(jnp.logical_or, here))(functools.partial(work, value))

    def rows(k, size=None):
        return pl.ds(pl.multiple_of(k * R, R), R if size is None else size)

    def wait_for(ref, sem):
        pltpu.make_async_copy(ref, ref, sem).wait()

    def load_own(size):
        start = pl.multiple_of(of(begin, x), 16)
        return pltpu.make_async_copy(sig.at[pl.ds(start, size)], row.at[x, :size], load_sem.at[2])

    barrier = pltpu.get_barrier_semaphore()

    def meet(condition, peer):
        @pl.when(condition)
        def _():
            pl.semaphore_signal(barrier, inc=1, device_id=peer, device_id_type=MESH)

    for c in range(1, X):
        meet(c > x, at_x(c))
    meet(y < Y - 1, at_y(along_y(1)))
    meet(y == 0, at_y(along_y(Y - 1)))

    loads = []
    for part in range(2):
        for c in range(X):
            start, stop = ((0, LEAD * R), (LEAD * R, share[c]))[part]
            piece = pl.ds(begin[c] + start, stop - start)
            loads.append(pltpu.make_async_copy(sig.at[piece], mine.at[piece], load_sem.at[part]))
    load_gain = pltpu.make_async_copy(gain_in, gain, load_sem.at[3])
    for load in loads:
        load.start()
    by_column(share, lambda size: load_own(size).start())
    load_gain.start()
    acc[...] = jnp.zeros_like(acc)
    met = x + jnp.where(y > 0, 1, 0) + jnp.where(y == Y - 1, 1, 0)

    @pl.when(met > 0)
    def _():
        pl.semaphore_wait(barrier, met)

    for c in range(X - 1):

        @pl.when(c < x)
        def _(c=c):
            pl.semaphore_signal(ready.at[x], inc=1, device_id=at_x(c), device_id_type=MESH)

    @pl.when(y > 0)
    def _():
        pl.semaphore_signal(ready.at[0], inc=1, device_id=at_y(along_y(Y - 1)), device_id_type=MESH)

    def send_in(c, k, size=None):
        start = pl.multiple_of((of(begin, c) if size is None else begin[c]) + k * R, 16)
        pltpu.make_async_remote_copy(
            src_ref=mine.at[pl.ds(start, R if size is None else size)],
            dst_ref=row.at[x, rows(k, size)],
            send_sem=in_send,
            recv_sem=in_recv.at[k],
            device_id=at_x(c),
            device_id_type=MESH,
        ).start()

    def send_up(c, k, size=None):
        pltpu.make_async_remote_copy(
            src_ref=row.at[c, rows(k, size)],
            dst_ref=below.at[c - 1, rows(k, size)],
            send_sem=up_send,
            recv_sem=up_recv.at[k],
            device_id=at_y(along_y(1)),
            device_id_type=MESH,
        ).start()

    def send_out(d, k, size=None):
        c = along_x(d)
        pltpu.make_async_remote_copy(
            src_ref=mixed.at[c, rows(k, size)],
            dst_ref=back.at[x, rows(k, size)],
            send_sem=out_send,
            recv_sem=out_recv.at[k],
            device_id=at_x(c),
            device_id_type=MESH,
        ).start()

    def three(ref, k, size=None):
        return ref.at[: X - 1, rows(k, size)]

    for load in loads[:X]:
        load.wait()
    for c in range(X - 1):
        for k in range(LEAD):

            @pl.when(c < x)
            def _(c=c, k=k):
                send_in(c, k)

    for c in range(1, X):

        @pl.when(c > x)
        def _(c=c):
            pl.semaphore_wait(ready.at[c], 1)
            for k in range(LEAD):
                send_in(c, k)

    for load in loads[X:]:
        load.wait()

    def to_others(k, whole):
        for c in (0, 2, 1, 3):

            @pl.when(x != c)
            def _(c=c):
                send_in(c, k, R if whole else tail[c])

    @pl.loop(LEAD, last)
    def _(k):
        to_others(k, True)

    to_others(last, False)
    by_column(share, lambda size: load_own(size).wait())

    @pl.when(y < Y - 1)
    def _():
        pl.semaphore_wait(ready.at[0], 1)

    @pl.when(x > 0)
    def _():
        @pl.loop(0, last)
        def _(k):
            send_up(x, k)

        by_column(tail, lambda size: send_up(x, last, size))

    load_gain.wait()

    def gather(k, size=None):
        wait_for(three(row, k, size), in_recv.at[k])
        for c in range(1, X):

            @pl.when(x != c)
            def _(c=c):
                send_up(c, k, size)

    def mix(k, size=None):
        size = R if size is None else size
        wait_for(three(below, k, size), up_recv.at[k])
        g0, g1, g2 = (jnp.broadcast_to(gain[i : i + 1, :], (8, gain.shape[1])) for i in range(3))

        def block(i, total):
            at = pl.ds(pl.multiple_of(k * R + i * BLOCK, BLOCK), BLOCK)
            taps = [below[c, at, :] for c in range(X - 1)] + [row[c, at, :] for c in range(X)]
            taps = [t.astype(jnp.float32).reshape(BLOCK // 8, 8, -1) for t in taps]
            for c in range(X):
                m = g0 * taps[c + 3] + g1 * taps[c + 1] + g2 * taps[c]
                total = total + jnp.sum(m * m, axis=0)
                mixed[c, at, :] = m.reshape(BLOCK, -1).astype(jnp.bfloat16)
            return total

        acc[...] = lax.fori_loop(0, size // BLOCK, block, acc[...])

    def give_back(k, size=None):
        for d in (2, 1, 3):
            send_out(d, k, size)

    gather(0)

    @pl.loop(1, EARLY + 1)
    def _(k):
        gather(k)
        mix(k - 1)
        give_back(k - 1)

    @pl.loop(EARLY + 1, last)
    def _(k):
        gather(k)
        mix(k - 1)

    by_column(tail, lambda size: gather(last, size))
    mix(last - 1)
    by_column(tail, lambda size: mix(last, size))

    for d in range(1, Y):
        pltpu.make_async_remote_copy(
            src_ref=acc, dst_ref=part_y.at[d - 1], send_sem=power_send.at[0], recv_sem=power_recv.at[0],
            device_id=at_y(along_y(d)), device_id_type=MESH,
        ).start()
    wait_for(part_y, power_recv.at[0])
    sum_y[...] = acc[...] + jnp.sum(part_y[...], axis=0)
    for d in range(1, X):
        pltpu.make_async_remote_copy(
            src_ref=sum_y, dst_ref=part_x.at[d - 1], send_sem=power_send.at[1], recv_sem=power_recv.at[1],
            device_id=at_x(along_x(d)), device_id_type=MESH,
        ).start()

    @pl.loop(EARLY, last)
    def _(k):
        give_back(k)

    by_column(tail, lambda size: give_back(last, size))

    wait_for(part_x, power_recv.at[1])
    total = sum_y[...] + jnp.sum(part_x[...], axis=0)
    power = jnp.sum(total, axis=0, keepdims=True) / (X * even * phases)
    scale = jnp.broadcast_to(lax.rsqrt(power + 1e-05), (8, out.shape[1]))

    def finish(source, c, begins, start, size):
        m = source[c, pl.ds(start, size), :].astype(jnp.float32).reshape(size // 8, 8, -1) * scale
        at = pl.ds(pl.multiple_of(begins + start, 16), size)
        out[at, :] = m.reshape(size, -1).astype(jnp.bfloat16)

    def finish_piece(source, c, k):
        begins = of(begin, c)

        @pl.loop(0, R // WIDE)
        def _(i):
            finish(source, c, begins, pl.multiple_of(k * R + i * WIDE, 16), WIDE)

    @pl.loop(0, last)
    def _(k):
        finish_piece(mixed, x, k)

    by_column(tail, lambda size: finish(mixed, x, of(begin, x), last * R, size))

    @pl.loop(0, last)
    def _(k):
        wait_for(three(back, k), out_recv.at[k])
        for d in range(1, X):
            finish_piece(back, along_x(d), k)

    by_column([sum(tail) - t for t in tail], lambda n: wait_for(mine.at[:n], out_recv.at[last]))
    for c in range(X):

        @pl.when(x != c)
        def _(c=c):
            finish(back, c, begin[c], last * R, tail[c])

    by_column([sum(share) - t for t in share], lambda n: wait_for(mine.at[:n], in_send))
    by_column(share, lambda size: wait_for(below.at[:, :size], up_send))
    by_column(share, lambda size: wait_for(below.at[:, :size], out_send))
    wait_for(part_y, power_send.at[0])
    wait_for(part_x, power_send.at[1])


def body(signal, tap_gain):
    steps, channels = signal.shape[2:]
    Y = lax.axis_size("phase") // X
    part = steps // X + max(SHIFT)
    pieces = whole_pieces(steps // X) + 1
    dma = pltpu.SemaphoreType.DMA

    def rows(n):
        return pltpu.VMEM((n, part, channels), jnp.bfloat16)

    def sums(*n):
        return pltpu.VMEM((*n, 8, channels), jnp.float32)

    out = pl.pallas_call(
        kernel,
        name="echoes",
        out_shape=pltpu.VMEM((steps, channels), signal.dtype),
        in_specs=[pl.BlockSpec(memory_space=pltpu.HBM)] * 2,
        out_specs=pl.BlockSpec(memory_space=pltpu.VMEM),
        scratch_shapes=[
            pltpu.VMEM(tap_gain.shape, jnp.float32),
            pltpu.VMEM((steps, channels), jnp.bfloat16),
            rows(X),
            rows(X - 1),
            rows(X),
            rows(X),
            sums(),
            sums(X - 1),
            sums(Y - 1),
            sums(),
            pltpu.SemaphoreType.REGULAR((X,)),
            dma((4,)),
            dma(()),
            dma((pieces,)),
            dma(()),
            dma((pieces,)),
            dma(()),
            dma((pieces,)),
            dma((2,)),
            dma((2,)),
        ],
        compiler_params=pltpu.CompilerParams(
            collective_id=0, has_side_effects=True, vmem_limit_bytes=VMEM
        ),
    )(signal.reshape(steps, channels), tap_gain)
    return out.reshape(signal.shape)


def solution(mesh):
    return jax.shard_map(
        body,
        mesh=mesh,
        in_specs=(P("phase", "line", None, None), P()),
        out_specs=P("phase", "line", None, None),
        check_vma=False,
    )
```

```python
import functools

import jax
import jax.numpy as jnp
from jax import lax
from jax.experimental import pallas as pl
from jax.experimental.pallas import tpu as pltpu
from jax.sharding import PartitionSpec as P

MESH = pl.DeviceIdType.MESH
X = 4
ROWS = 240
LAG = 1
SHIFT = (-32, 32, 48, -48)
EARLY = 7
LEAD = 1
BLOCK = 16
WIDE = 80
ORDER = (2, 3, 1)
MIB = 2**20
VMEM = 54 * MIB


def whole_pieces(even):
    return (even + min(SHIFT) - 1) // ROWS


def kernel(
    sig, gain_in, out, gain, mine, row, below, mixed, back, acc, part_x, part_y, sum_y,
    ready, load_sem, in_send, in_recv, up_send, up_recv, out_send, out_recv, power_send, power_recv,
):
    me = lax.axis_index("phase")
    phases = lax.axis_size("phase")
    Y = phases // X
    x, y = lax.rem(me, X), me // X
    even = out.shape[0] // X
    R, last = ROWS, whole_pieces(even)
    share = [even + SHIFT[c] for c in range(X)]
    begin = [sum(share[:c]) for c in range(X)]
    tail = [share[c] - last * R for c in range(X)]

    def along_x(d):
        return lax.rem(x + d, X)

    def along_y(d):
        return lax.rem(y + d, Y)

    def at_x(c):
        return {"phase": y * X + c}

    def at_y(r):
        return {"phase": r * X + x}

    def of(values, c):
        picked = jnp.int32(values[0])
        for i in range(1, X):
            picked = jnp.where(c == i, values[i], picked)
        return picked

    def by_column(values, work):
        for value in sorted(set(values)):
            here = [x == c for c in range(X) if values[c] == value]
            pl.when(functools.reduce(jnp.logical_or, here))(functools.partial(work, value))

    def rows(k, size=None):
        return pl.ds(pl.multiple_of(k * R, R), R if size is None else size)

    def wait_for(ref, sem):
        pltpu.make_async_copy(ref, ref, sem).wait()

    def load_own(size):
        start = pl.multiple_of(of(begin, x), 16)
        return pltpu.make_async_copy(sig.at[pl.ds(start, size)], row.at[x, :size], load_sem.at[2])

    barrier = pltpu.get_barrier_semaphore()

    def meet(condition, peer):
        @pl.when(condition)
        def _():
            pl.semaphore_signal(barrier, inc=1, device_id=peer, device_id_type=MESH)

    for c in range(1, X):
        meet(c > x, at_x(c))
    meet(y < Y - 1, at_y(along_y(1)))
    meet(y == 0, at_y(along_y(Y - 1)))

    loads = []
    for part in range(2):
        for c in range(X):
            start, stop = ((0, LEAD * R), (LEAD * R, share[c]))[part]
            piece = pl.ds(begin[c] + start, stop - start)
            loads.append(pltpu.make_async_copy(sig.at[piece], mine.at[piece], load_sem.at[part]))
    load_gain = pltpu.make_async_copy(gain_in, gain, load_sem.at[3])
    for load in loads:
        load.start()
    by_column(share, lambda size: load_own(size).start())
    load_gain.start()
    acc[...] = jnp.zeros_like(acc)
    met = x + jnp.where(y > 0, 1, 0) + jnp.where(y == Y - 1, 1, 0)

    @pl.when(met > 0)
    def _():
        pl.semaphore_wait(barrier, met)

    for c in range(X - 1):

        @pl.when(c < x)
        def _(c=c):
            pl.semaphore_signal(ready.at[x], inc=1, device_id=at_x(c), device_id_type=MESH)

    @pl.when(y > 0)
    def _():
        pl.semaphore_signal(ready.at[0], inc=1, device_id=at_y(along_y(Y - 1)), device_id_type=MESH)

    def send_in(c, k, size=None):
        start = pl.multiple_of((of(begin, c) if size is None else begin[c]) + k * R, 16)
        pltpu.make_async_remote_copy(
            src_ref=mine.at[pl.ds(start, R if size is None else size)],
            dst_ref=row.at[x, rows(k, size)],
            send_sem=in_send,
            recv_sem=in_recv.at[k],
            device_id=at_x(c),
            device_id_type=MESH,
        ).start()

    def send_up(c, k, size=None):
        pltpu.make_async_remote_copy(
            src_ref=row.at[c, rows(k, size)],
            dst_ref=below.at[c - 1, rows(k, size)],
            send_sem=up_send,
            recv_sem=up_recv.at[k],
            device_id=at_y(along_y(1)),
            device_id_type=MESH,
        ).start()

    def send_out(d, k, size=None):
        c = along_x(d)
        pltpu.make_async_remote_copy(
            src_ref=mixed.at[c, rows(k, size)],
            dst_ref=back.at[x, rows(k, size)],
            send_sem=out_send,
            recv_sem=out_recv.at[k],
            device_id=at_x(c),
            device_id_type=MESH,
        ).start()

    def three(ref, k, size=None):
        return ref.at[: X - 1, rows(k, size)]

    for load in loads[:X]:
        load.wait()
    for c in range(X - 1):
        for k in range(LEAD):

            @pl.when(c < x)
            def _(c=c, k=k):
                send_in(c, k)

    for c in range(1, X):

        @pl.when(c > x)
        def _(c=c):
            pl.semaphore_wait(ready.at[c], 1)
            for k in range(LEAD):
                send_in(c, k)

    for load in loads[X:]:
        load.wait()

    def to_others(k, whole):
        for d in ORDER:
            for c in range(X):

                @pl.when(along_x(d) == c)
                def _(c=c):
                    send_in(c, k, R if whole else tail[c])

    @pl.loop(LEAD, last)
    def _(k):
        to_others(k, True)

    to_others(last, False)
    by_column(share, lambda size: load_own(size).wait())

    @pl.when(y < Y - 1)
    def _():
        pl.semaphore_wait(ready.at[0], 1)

    @pl.when(x > 0)
    def _():
        @pl.loop(0, last)
        def _(k):
            send_up(x, k)

        by_column(tail, lambda size: send_up(x, last, size))

    load_gain.wait()

    def gather(k, size=None):
        wait_for(three(row, k, size), in_recv.at[k])
        for c in range(1, X):

            @pl.when(x != c)
            def _(c=c):
                send_up(c, k, size)

    def mix(k, size=None):
        size = R if size is None else size
        wait_for(three(below, k, size), up_recv.at[k])
        g0, g1, g2 = (jnp.broadcast_to(gain[i : i + 1, :], (8, gain.shape[1])) for i in range(3))

        def block(i, total):
            at = pl.ds(pl.multiple_of(k * R + i * BLOCK, BLOCK), BLOCK)
            taps = [below[c, at, :] for c in range(X - 1)] + [row[c, at, :] for c in range(X)]
            taps = [t.astype(jnp.float32).reshape(BLOCK // 8, 8, -1) for t in taps]
            for c in range(X):
                m = g0 * taps[c + 3] + g1 * taps[c + 1] + g2 * taps[c]
                total = total + jnp.sum(m * m, axis=0)
                mixed[c, at, :] = m.reshape(BLOCK, -1).astype(jnp.bfloat16)
            return total

        acc[...] = lax.fori_loop(0, size // BLOCK, block, acc[...])

    def give_back(k, size=None):
        for d in ORDER:
            send_out(d, k, size)

    gather(0)

    @pl.loop(1, EARLY + 1)
    def _(k):
        gather(k)
        mix(k - 1)
        give_back(k - 1)

    @pl.loop(EARLY + 1, last)
    def _(k):
        gather(k)
        mix(k - 1)

    by_column(tail, lambda size: gather(last, size))
    mix(last - 1)
    by_column(tail, lambda size: mix(last, size))

    for d in range(1, Y):
        pltpu.make_async_remote_copy(
            src_ref=acc, dst_ref=part_y.at[d - 1], send_sem=power_send.at[0], recv_sem=power_recv.at[0],
            device_id=at_y(along_y(d)), device_id_type=MESH,
        ).start()
    wait_for(part_y, power_recv.at[0])
    sum_y[...] = acc[...] + jnp.sum(part_y[...], axis=0)
    for d in range(1, X):
        pltpu.make_async_remote_copy(
            src_ref=sum_y, dst_ref=part_x.at[d - 1], send_sem=power_send.at[1], recv_sem=power_recv.at[1],
            device_id=at_x(along_x(d)), device_id_type=MESH,
        ).start()

    @pl.loop(EARLY, last)
    def _(k):
        give_back(k)

    by_column(tail, lambda size: give_back(last, size))

    wait_for(part_x, power_recv.at[1])
    total = sum_y[...] + jnp.sum(part_x[...], axis=0)
    power = jnp.sum(total, axis=0, keepdims=True) / (X * even * phases)
    scale = jnp.broadcast_to(lax.rsqrt(power + 1e-05), (8, out.shape[1]))

    def finish(source, c, begins, start, size):
        m = source[c, pl.ds(start, size), :].astype(jnp.float32).reshape(size // 8, 8, -1) * scale
        at = pl.ds(pl.multiple_of(begins + start, 16), size)
        out[at, :] = m.reshape(size, -1).astype(jnp.bfloat16)

    def finish_piece(source, c, k):
        begins = of(begin, c)

        @pl.loop(0, R // WIDE)
        def _(i):
            finish(source, c, begins, pl.multiple_of(k * R + i * WIDE, 16), WIDE)

    @pl.loop(0, last)
    def _(k):
        finish_piece(mixed, x, k)

    by_column(tail, lambda size: finish(mixed, x, of(begin, x), last * R, size))

    @pl.loop(0, last)
    def _(k):
        wait_for(three(back, k), out_recv.at[k])
        for d in range(1, X):
            finish_piece(back, along_x(d), k)

    by_column([sum(tail) - t for t in tail], lambda n: wait_for(mine.at[:n], out_recv.at[last]))
    for c in range(X):

        @pl.when(x != c)
        def _(c=c):
            finish(back, c, begin[c], last * R, tail[c])

    by_column([sum(share) - t for t in share], lambda n: wait_for(mine.at[:n], in_send))
    by_column(share, lambda size: wait_for(below.at[:, :size], up_send))
    by_column(share, lambda size: wait_for(below.at[:, :size], out_send))
    wait_for(part_y, power_send.at[0])
    wait_for(part_x, power_send.at[1])


def body(signal, tap_gain):
    steps, channels = signal.shape[2:]
    Y = lax.axis_size("phase") // X
    part = steps // X + max(SHIFT)
    pieces = whole_pieces(steps // X) + 1
    dma = pltpu.SemaphoreType.DMA

    def rows(n):
        return pltpu.VMEM((n, part, channels), jnp.bfloat16)

    def sums(*n):
        return pltpu.VMEM((*n, 8, channels), jnp.float32)

    out = pl.pallas_call(
        kernel,
        name="echoes",
        out_shape=pltpu.VMEM((steps, channels), signal.dtype),
        in_specs=[pl.BlockSpec(memory_space=pltpu.HBM)] * 2,
        out_specs=pl.BlockSpec(memory_space=pltpu.VMEM),
        scratch_shapes=[
            pltpu.VMEM(tap_gain.shape, jnp.float32),
            pltpu.VMEM((steps, channels), jnp.bfloat16),
            rows(X),
            rows(X - 1),
            rows(X),
            rows(X),
            sums(),
            sums(X - 1),
            sums(Y - 1),
            sums(),
            pltpu.SemaphoreType.REGULAR((X,)),
            dma((4,)),
            dma(()),
            dma((pieces,)),
            dma(()),
            dma((pieces,)),
            dma(()),
            dma((pieces,)),
            dma((2,)),
            dma((2,)),
        ],
        compiler_params=pltpu.CompilerParams(
            collective_id=0, has_side_effects=True, vmem_limit_bytes=VMEM
        ),
    )(signal.reshape(steps, channels), tap_gain)
    return out.reshape(signal.shape)


def solution(mesh):
    return jax.shard_map(
        body,
        mesh=mesh,
        in_specs=(P("phase", "line", None, None), P()),
        out_specs=P("phase", "line", None, None),
        check_vma=False,
    )
```

```python
import functools

import jax
import jax.numpy as jnp
from jax import lax
from jax.experimental import pallas as pl
from jax.experimental.pallas import tpu as pltpu
from jax.sharding import PartitionSpec as P

MESH = pl.DeviceIdType.MESH
X = 4
ROWS = 320
LAG = 1
SHIFT = (-32, 32, 48, -48)
EARLY = 5
LEAD = 1
BLOCK = 16
WIDE = 160
MIB = 2**20
VMEM = 54 * MIB


def whole_pieces(even):
    return (even + min(SHIFT) - 1) // ROWS


def kernel(
    sig, gain_in, out, gain, mine, row, below, mixed, back, acc, part_x, part_y, sum_y,
    ready, load_sem, in_send, in_recv, up_send, up_recv, out_send, out_recv, power_send, power_recv,
):
    me = lax.axis_index("phase")
    phases = lax.axis_size("phase")
    Y = phases // X
    x, y = lax.rem(me, X), me // X
    even = out.shape[0] // X
    R, last = ROWS, whole_pieces(even)
    share = [even + SHIFT[c] for c in range(X)]
    begin = [sum(share[:c]) for c in range(X)]
    tail = [share[c] - last * R for c in range(X)]

    def along_x(d):
        return lax.rem(x + d, X)

    def along_y(d):
        return lax.rem(y + d, Y)

    def at_x(c):
        return {"phase": y * X + c}

    def at_y(r):
        return {"phase": r * X + x}

    def of(values, c):
        picked = jnp.int32(values[0])
        for i in range(1, X):
            picked = jnp.where(c == i, values[i], picked)
        return picked

    def by_column(values, work):
        for value in sorted(set(values)):
            here = [x == c for c in range(X) if values[c] == value]
            pl.when(functools.reduce(jnp.logical_or, here))(functools.partial(work, value))

    def rows(k, size=None):
        return pl.ds(pl.multiple_of(k * R, R), R if size is None else size)

    def wait_for(ref, sem):
        pltpu.make_async_copy(ref, ref, sem).wait()

    def load_own(size):
        start = pl.multiple_of(of(begin, x), 16)
        return pltpu.make_async_copy(sig.at[pl.ds(start, size)], row.at[x, :size], load_sem.at[2])

    barrier = pltpu.get_barrier_semaphore()

    def meet(condition, peer):
        @pl.when(condition)
        def _():
            pl.semaphore_signal(barrier, inc=1, device_id=peer, device_id_type=MESH)

    for c in range(1, X):
        meet(c > x, at_x(c))
    meet(y < Y - 1, at_y(along_y(1)))
    meet(y == 0, at_y(along_y(Y - 1)))

    loads = []
    for part in range(2):
        for c in range(X):
            start, stop = ((0, LEAD * R), (LEAD * R, share[c]))[part]
            piece = pl.ds(begin[c] + start, stop - start)
            loads.append(pltpu.make_async_copy(sig.at[piece], mine.at[piece], load_sem.at[part]))
    load_gain = pltpu.make_async_copy(gain_in, gain, load_sem.at[3])
    for load in loads:
        load.start()
    by_column(share, lambda size: load_own(size).start())
    load_gain.start()
    acc[...] = jnp.zeros_like(acc)
    met = x + jnp.where(y > 0, 1, 0) + jnp.where(y == Y - 1, 1, 0)

    @pl.when(met > 0)
    def _():
        pl.semaphore_wait(barrier, met)

    for c in range(X - 1):

        @pl.when(c < x)
        def _(c=c):
            pl.semaphore_signal(ready.at[x], inc=1, device_id=at_x(c), device_id_type=MESH)

    @pl.when(y > 0)
    def _():
        pl.semaphore_signal(ready.at[0], inc=1, device_id=at_y(along_y(Y - 1)), device_id_type=MESH)

    def send_in(c, k, size=None):
        start = pl.multiple_of((of(begin, c) if size is None else begin[c]) + k * R, 16)
        pltpu.make_async_remote_copy(
            src_ref=mine.at[pl.ds(start, R if size is None else size)],
            dst_ref=row.at[x, rows(k, size)],
            send_sem=in_send,
            recv_sem=in_recv.at[k],
            device_id=at_x(c),
            device_id_type=MESH,
        ).start()

    def send_up(c, k, size=None):
        pltpu.make_async_remote_copy(
            src_ref=row.at[c, rows(k, size)],
            dst_ref=below.at[c - 1, rows(k, size)],
            send_sem=up_send,
            recv_sem=up_recv.at[k],
            device_id=at_y(along_y(1)),
            device_id_type=MESH,
        ).start()

    def send_out(d, k, size=None):
        c = along_x(d)
        pltpu.make_async_remote_copy(
            src_ref=mixed.at[c, rows(k, size)],
            dst_ref=back.at[x, rows(k, size)],
            send_sem=out_send,
            recv_sem=out_recv.at[k],
            device_id=at_x(c),
            device_id_type=MESH,
        ).start()

    def three(ref, k, size=None):
        return ref.at[: X - 1, rows(k, size)]

    for load in loads[:X]:
        load.wait()
    for c in range(X - 1):
        for k in range(LEAD):

            @pl.when(c < x)
            def _(c=c, k=k):
                send_in(c, k)

    for c in range(1, X):

        @pl.when(c > x)
        def _(c=c):
            pl.semaphore_wait(ready.at[c], 1)
            for k in range(LEAD):
                send_in(c, k)

    for load in loads[X:]:
        load.wait()

    def to_others(k, whole):
        for c in (0, 2, 1, 3):

            @pl.when(x != c)
            def _(c=c):
                send_in(c, k, R if whole else tail[c])

    @pl.loop(LEAD, last)
    def _(k):
        to_others(k, True)

    to_others(last, False)
    by_column(share, lambda size: load_own(size).wait())

    @pl.when(y < Y - 1)
    def _():
        pl.semaphore_wait(ready.at[0], 1)

    @pl.when(x > 0)
    def _():
        @pl.loop(0, last)
        def _(k):
            send_up(x, k)

        by_column(tail, lambda size: send_up(x, last, size))

    load_gain.wait()

    def gather(k, size=None):
        wait_for(three(row, k, size), in_recv.at[k])
        for c in range(1, X):

            @pl.when(x != c)
            def _(c=c):
                send_up(c, k, size)

    def mix(k, size=None):
        size = R if size is None else size
        wait_for(three(below, k, size), up_recv.at[k])
        g0, g1, g2 = (jnp.broadcast_to(gain[i : i + 1, :], (8, gain.shape[1])) for i in range(3))

        def block(i, total):
            at = pl.ds(pl.multiple_of(k * R + i * BLOCK, BLOCK), BLOCK)
            taps = [below[c, at, :] for c in range(X - 1)] + [row[c, at, :] for c in range(X)]
            taps = [t.astype(jnp.float32).reshape(BLOCK // 8, 8, -1) for t in taps]
            for c in range(X):
                m = g0 * taps[c + 3] + g1 * taps[c + 1] + g2 * taps[c]
                total = total + jnp.sum(m * m, axis=0)
                mixed[c, at, :] = m.reshape(BLOCK, -1).astype(jnp.bfloat16)
            return total

        acc[...] = lax.fori_loop(0, size // BLOCK, block, acc[...])

    def give_back(k, size=None):
        for d in (2, 1, 3):
            send_out(d, k, size)

    gather(0)

    @pl.loop(1, EARLY + 1)
    def _(k):
        gather(k)
        mix(k - 1)
        give_back(k - 1)

    @pl.loop(EARLY + 1, last)
    def _(k):
        gather(k)
        mix(k - 1)

    by_column(tail, lambda size: gather(last, size))
    mix(last - 1)
    by_column(tail, lambda size: mix(last, size))

    for d in range(1, Y):
        pltpu.make_async_remote_copy(
            src_ref=acc, dst_ref=part_y.at[d - 1], send_sem=power_send.at[0], recv_sem=power_recv.at[0],
            device_id=at_y(along_y(d)), device_id_type=MESH,
        ).start()
    wait_for(part_y, power_recv.at[0])
    sum_y[...] = acc[...] + jnp.sum(part_y[...], axis=0)
    for d in range(1, X):
        pltpu.make_async_remote_copy(
            src_ref=sum_y, dst_ref=part_x.at[d - 1], send_sem=power_send.at[1], recv_sem=power_recv.at[1],
            device_id=at_x(along_x(d)), device_id_type=MESH,
        ).start()

    @pl.loop(EARLY, last)
    def _(k):
        give_back(k)

    by_column(tail, lambda size: give_back(last, size))

    wait_for(part_x, power_recv.at[1])
    total = sum_y[...] + jnp.sum(part_x[...], axis=0)
    power = jnp.sum(total, axis=0, keepdims=True) / (X * even * phases)
    scale = jnp.broadcast_to(lax.rsqrt(power + 1e-05), (8, out.shape[1]))

    def finish(source, c, begins, start, size):
        m = source[c, pl.ds(start, size), :].astype(jnp.float32).reshape(size // 8, 8, -1) * scale
        at = pl.ds(pl.multiple_of(begins + start, 16), size)
        out[at, :] = m.reshape(size, -1).astype(jnp.bfloat16)

    def finish_piece(source, c, k):
        begins = of(begin, c)

        @pl.loop(0, R // WIDE)
        def _(i):
            finish(source, c, begins, pl.multiple_of(k * R + i * WIDE, 16), WIDE)

    @pl.loop(0, last)
    def _(k):
        finish_piece(mixed, x, k)

    by_column(tail, lambda size: finish(mixed, x, of(begin, x), last * R, size))

    @pl.loop(0, last)
    def _(k):
        wait_for(three(back, k), out_recv.at[k])
        for d in range(1, X):
            finish_piece(back, along_x(d), k)

    by_column([sum(tail) - t for t in tail], lambda n: wait_for(mine.at[:n], out_recv.at[last]))
    for c in range(X):

        @pl.when(x != c)
        def _(c=c):
            finish(back, c, begin[c], last * R, tail[c])

    by_column([sum(share) - t for t in share], lambda n: wait_for(mine.at[:n], in_send))
    by_column(share, lambda size: wait_for(below.at[:, :size], up_send))
    by_column(share, lambda size: wait_for(below.at[:, :size], out_send))
    wait_for(part_y, power_send.at[0])
    wait_for(part_x, power_send.at[1])


def body(signal, tap_gain):
    steps, channels = signal.shape[2:]
    Y = lax.axis_size("phase") // X
    part = steps // X + max(SHIFT)
    pieces = whole_pieces(steps // X) + 1
    dma = pltpu.SemaphoreType.DMA

    def rows(n):
        return pltpu.VMEM((n, part, channels), jnp.bfloat16)

    def sums(*n):
        return pltpu.VMEM((*n, 8, channels), jnp.float32)

    out = pl.pallas_call(
        kernel,
        name="echoes",
        out_shape=pltpu.VMEM((steps, channels), signal.dtype),
        in_specs=[pl.BlockSpec(memory_space=pltpu.HBM)] * 2,
        out_specs=pl.BlockSpec(memory_space=pltpu.VMEM),
        scratch_shapes=[
            pltpu.VMEM(tap_gain.shape, jnp.float32),
            pltpu.VMEM((steps, channels), jnp.bfloat16),
            rows(X),
            rows(X - 1),
            rows(X),
            rows(X),
            sums(),
            sums(X - 1),
            sums(Y - 1),
            sums(),
            pltpu.SemaphoreType.REGULAR((X,)),
            dma((4,)),
            dma(()),
            dma((pieces,)),
            dma(()),
            dma((pieces,)),
            dma(()),
            dma((pieces,)),
            dma((2,)),
            dma((2,)),
        ],
        compiler_params=pltpu.CompilerParams(
            collective_id=0, has_side_effects=True, vmem_limit_bytes=VMEM
        ),
    )(signal.reshape(steps, channels), tap_gain)
    return out.reshape(signal.shape)


def solution(mesh):
    return jax.shard_map(
        body,
        mesh=mesh,
        in_specs=(P("phase", "line", None, None), P()),
        out_specs=P("phase", "line", None, None),
        check_vma=False,
    )
```

```python
import functools

import jax
import jax.numpy as jnp
from jax import lax
from jax.experimental import pallas as pl
from jax.experimental.pallas import tpu as pltpu
from jax.sharding import PartitionSpec as P

MESH = pl.DeviceIdType.MESH
X = 4
ROWS = 224
LAG = 1
SHIFT = (-32, 32, 48, -48)
EARLY = 7
LEAD = 1
BLOCK = 16
WIDE = 112
MIB = 2**20
VMEM = 54 * MIB


def whole_pieces(even):
    return (even + min(SHIFT) - 1) // ROWS


def kernel(
    sig, gain_in, out, gain, mine, row, below, mixed, back, acc, part_x, part_y, sum_y,
    ready, load_sem, in_send, in_recv, up_send, up_recv, out_send, out_recv, power_send, power_recv,
):
    me = lax.axis_index("phase")
    phases = lax.axis_size("phase")
    Y = phases // X
    x, y = lax.rem(me, X), me // X
    even = out.shape[0] // X
    R, last = ROWS, whole_pieces(even)
    share = [even + SHIFT[c] for c in range(X)]
    begin = [sum(share[:c]) for c in range(X)]
    tail = [share[c] - last * R for c in range(X)]

    def along_x(d):
        return lax.rem(x + d, X)

    def along_y(d):
        return lax.rem(y + d, Y)

    def at_x(c):
        return {"phase": y * X + c}

    def at_y(r):
        return {"phase": r * X + x}

    def of(values, c):
        picked = jnp.int32(values[0])
        for i in range(1, X):
            picked = jnp.where(c == i, values[i], picked)
        return picked

    def by_column(values, work):
        for value in sorted(set(values)):
            here = [x == c for c in range(X) if values[c] == value]
            pl.when(functools.reduce(jnp.logical_or, here))(functools.partial(work, value))

    def rows(k, size=None):
        return pl.ds(pl.multiple_of(k * R, R), R if size is None else size)

    def wait_for(ref, sem):
        pltpu.make_async_copy(ref, ref, sem).wait()

    def load_own(size):
        start = pl.multiple_of(of(begin, x), 16)
        return pltpu.make_async_copy(sig.at[pl.ds(start, size)], row.at[x, :size], load_sem.at[2])

    barrier = pltpu.get_barrier_semaphore()

    def meet(condition, peer):
        @pl.when(condition)
        def _():
            pl.semaphore_signal(barrier, inc=1, device_id=peer, device_id_type=MESH)

    for c in range(1, X):
        meet(c > x, at_x(c))
    meet(y < Y - 1, at_y(along_y(1)))
    meet(y == 0, at_y(along_y(Y - 1)))

    loads = []
    for part in range(2):
        for c in range(X):
            start, stop = ((0, LEAD * R), (LEAD * R, share[c]))[part]
            piece = pl.ds(begin[c] + start, stop - start)
            loads.append(pltpu.make_async_copy(sig.at[piece], mine.at[piece], load_sem.at[part]))
    load_gain = pltpu.make_async_copy(gain_in, gain, load_sem.at[3])
    for load in loads:
        load.start()
    by_column(share, lambda size: load_own(size).start())
    load_gain.start()
    acc[...] = jnp.zeros_like(acc)
    met = x + jnp.where(y > 0, 1, 0) + jnp.where(y == Y - 1, 1, 0)

    @pl.when(met > 0)
    def _():
        pl.semaphore_wait(barrier, met)

    for c in range(X - 1):

        @pl.when(c < x)
        def _(c=c):
            pl.semaphore_signal(ready.at[x], inc=1, device_id=at_x(c), device_id_type=MESH)

    @pl.when(y > 0)
    def _():
        pl.semaphore_signal(ready.at[0], inc=1, device_id=at_y(along_y(Y - 1)), device_id_type=MESH)

    def send_in(c, k, size=None):
        start = pl.multiple_of((of(begin, c) if size is None else begin[c]) + k * R, 16)
        pltpu.make_async_remote_copy(
            src_ref=mine.at[pl.ds(start, R if size is None else size)],
            dst_ref=row.at[x, rows(k, size)],
            send_sem=in_send,
            recv_sem=in_recv.at[k],
            device_id=at_x(c),
            device_id_type=MESH,
        ).start()

    def send_up(c, k, size=None):
        pltpu.make_async_remote_copy(
            src_ref=row.at[c, rows(k, size)],
            dst_ref=below.at[c - 1, rows(k, size)],
            send_sem=up_send,
            recv_sem=up_recv.at[k],
            device_id=at_y(along_y(1)),
            device_id_type=MESH,
        ).start()

    def send_out(d, k, size=None):
        c = along_x(d)
        pltpu.make_async_remote_copy(
            src_ref=mixed.at[c, rows(k, size)],
            dst_ref=back.at[x, rows(k, size)],
            send_sem=out_send,
            recv_sem=out_recv.at[k],
            device_id=at_x(c),
            device_id_type=MESH,
        ).start()

    def three(ref, k, size=None):
        return ref.at[: X - 1, rows(k, size)]

    for load in loads[:X]:
        load.wait()
    for c in range(X - 1):
        for k in range(LEAD):

            @pl.when(c < x)
            def _(c=c, k=k):
                send_in(c, k)

    for c in range(1, X):

        @pl.when(c > x)
        def _(c=c):
            pl.semaphore_wait(ready.at[c], 1)
            for k in range(LEAD):
                send_in(c, k)

    for load in loads[X:]:
        load.wait()

    def to_others(k, whole):
        for c in (0, 2, 1, 3):

            @pl.when(x != c)
            def _(c=c):
                send_in(c, k, R if whole else tail[c])

    @pl.loop(LEAD, last)
    def _(k):
        to_others(k, True)

    to_others(last, False)
    by_column(share, lambda size: load_own(size).wait())

    @pl.when(y < Y - 1)
    def _():
        pl.semaphore_wait(ready.at[0], 1)

    @pl.when(x > 0)
    def _():
        @pl.loop(0, last)
        def _(k):
            send_up(x, k)

        by_column(tail, lambda size: send_up(x, last, size))

    load_gain.wait()

    def gather(k, size=None):
        wait_for(three(row, k, size), in_recv.at[k])
        for c in range(1, X):

            @pl.when(x != c)
            def _(c=c):
                send_up(c, k, size)

    def mix(k, size=None):
        size = R if size is None else size
        wait_for(three(below, k, size), up_recv.at[k])
        g0, g1, g2 = (jnp.broadcast_to(gain[i : i + 1, :], (8, gain.shape[1])) for i in range(3))

        def block(i, total):
            at = pl.ds(pl.multiple_of(k * R + i * BLOCK, BLOCK), BLOCK)
            taps = [below[c, at, :] for c in range(X - 1)] + [row[c, at, :] for c in range(X)]
            taps = [t.astype(jnp.float32).reshape(BLOCK // 8, 8, -1) for t in taps]
            for c in range(X):
                m = g0 * taps[c + 3] + g1 * taps[c + 1] + g2 * taps[c]
                total = total + jnp.sum(m * m, axis=0)
                mixed[c, at, :] = m.reshape(BLOCK, -1).astype(jnp.bfloat16)
            return total

        acc[...] = lax.fori_loop(0, size // BLOCK, block, acc[...])

    def give_back(k, size=None):
        for d in (2, 1, 3):
            send_out(d, k, size)

    gather(0)

    @pl.loop(1, EARLY + 1)
    def _(k):
        gather(k)
        mix(k - 1)
        give_back(k - 1)

    @pl.loop(EARLY + 1, last)
    def _(k):
        gather(k)
        mix(k - 1)

    by_column(tail, lambda size: gather(last, size))
    mix(last - 1)
    by_column(tail, lambda size: mix(last, size))

    for d in range(1, Y):
        pltpu.make_async_remote_copy(
            src_ref=acc, dst_ref=part_y.at[d - 1], send_sem=power_send.at[0], recv_sem=power_recv.at[0],
            device_id=at_y(along_y(d)), device_id_type=MESH,
        ).start()
    wait_for(part_y, power_recv.at[0])
    sum_y[...] = acc[...] + jnp.sum(part_y[...], axis=0)
    for d in range(1, X):
        pltpu.make_async_remote_copy(
            src_ref=sum_y, dst_ref=part_x.at[d - 1], send_sem=power_send.at[1], recv_sem=power_recv.at[1],
            device_id=at_x(along_x(d)), device_id_type=MESH,
        ).start()

    @pl.loop(EARLY, last)
    def _(k):
        give_back(k)

    by_column(tail, lambda size: give_back(last, size))

    wait_for(part_x, power_recv.at[1])
    total = sum_y[...] + jnp.sum(part_x[...], axis=0)
    power = jnp.sum(total, axis=0, keepdims=True) / (X * even * phases)
    scale = jnp.broadcast_to(lax.rsqrt(power + 1e-05), (8, out.shape[1]))

    def finish(source, c, begins, start, size):
        m = source[c, pl.ds(start, size), :].astype(jnp.float32).reshape(size // 8, 8, -1) * scale
        at = pl.ds(pl.multiple_of(begins + start, 16), size)
        out[at, :] = m.reshape(size, -1).astype(jnp.bfloat16)

    def finish_piece(source, c, k):
        begins = of(begin, c)

        @pl.loop(0, R // WIDE)
        def _(i):
            finish(source, c, begins, pl.multiple_of(k * R + i * WIDE, 16), WIDE)

    @pl.loop(0, last)
    def _(k):
        finish_piece(mixed, x, k)

    by_column(tail, lambda size: finish(mixed, x, of(begin, x), last * R, size))

    @pl.loop(0, last)
    def _(k):
        wait_for(three(back, k), out_recv.at[k])
        for d in range(1, X):
            finish_piece(back, along_x(d), k)

    by_column([sum(tail) - t for t in tail], lambda n: wait_for(mine.at[:n], out_recv.at[last]))
    for c in range(X):

        @pl.when(x != c)
        def _(c=c):
            finish(back, c, begin[c], last * R, tail[c])

    by_column([sum(share) - t for t in share], lambda n: wait_for(mine.at[:n], in_send))
    by_column(share, lambda size: wait_for(below.at[:, :size], up_send))
    by_column(share, lambda size: wait_for(below.at[:, :size], out_send))
    wait_for(part_y, power_send.at[0])
    wait_for(part_x, power_send.at[1])


def body(signal, tap_gain):
    steps, channels = signal.shape[2:]
    Y = lax.axis_size("phase") // X
    part = steps // X + max(SHIFT)
    pieces = whole_pieces(steps // X) + 1
    dma = pltpu.SemaphoreType.DMA

    def rows(n):
        return pltpu.VMEM((n, part, channels), jnp.bfloat16)

    def sums(*n):
        return pltpu.VMEM((*n, 8, channels), jnp.float32)

    out = pl.pallas_call(
        kernel,
        name="echoes",
        out_shape=pltpu.VMEM((steps, channels), signal.dtype),
        in_specs=[pl.BlockSpec(memory_space=pltpu.HBM)] * 2,
        out_specs=pl.BlockSpec(memory_space=pltpu.VMEM),
        scratch_shapes=[
            pltpu.VMEM(tap_gain.shape, jnp.float32),
            pltpu.VMEM((steps, channels), jnp.bfloat16),
            rows(X),
            rows(X - 1),
            rows(X),
            rows(X),
            sums(),
            sums(X - 1),
            sums(Y - 1),
            sums(),
            pltpu.SemaphoreType.REGULAR((X,)),
            dma((4,)),
            dma(()),
            dma((pieces,)),
            dma(()),
            dma((pieces,)),
            dma(()),
            dma((pieces,)),
            dma((2,)),
            dma((2,)),
        ],
        compiler_params=pltpu.CompilerParams(
            collective_id=0, has_side_effects=True, vmem_limit_bytes=VMEM
        ),
    )(signal.reshape(steps, channels), tap_gain)
    return out.reshape(signal.shape)


def solution(mesh):
    return jax.shard_map(
        body,
        mesh=mesh,
        in_specs=(P("phase", "line", None, None), P()),
        out_specs=P("phase", "line", None, None),
        check_vma=False,
    )
```

```python
import functools

import jax
import jax.numpy as jnp
from jax import lax
from jax.experimental import pallas as pl
from jax.experimental.pallas import tpu as pltpu
from jax.sharding import PartitionSpec as P

MESH = pl.DeviceIdType.MESH
X = 4
ROWS = 240
LAG = 1
SHIFT = (-32, 32, 48, -48)
EARLY = 7
LEAD = 1
BLOCK = 16
WIDE = 80
MIB = 2**20
VMEM = 54 * MIB


def whole_pieces(even):
    return (even + min(SHIFT) - 1) // ROWS


def kernel(
    sig, gain_in, out, gain, mine, row, below, mixed, back, acc, part_x, part_y, sum_y,
    ready, load_sem, in_send, in_recv, up_send, up_recv, out_send, out_recv, power_send, power_recv,
):
    me = lax.axis_index("phase")
    phases = lax.axis_size("phase")
    Y = phases // X
    x, y = lax.rem(me, X), me // X
    even = out.shape[0] // X
    R, last = ROWS, whole_pieces(even)
    share = [even + SHIFT[c] for c in range(X)]
    begin = [sum(share[:c]) for c in range(X)]
    tail = [share[c] - last * R for c in range(X)]

    def along_x(d):
        return lax.rem(x + d, X)

    def along_y(d):
        return lax.rem(y + d, Y)

    def at_x(c):
        return {"phase": y * X + c}

    def at_y(r):
        return {"phase": r * X + x}

    def of(values, c):
        picked = jnp.int32(values[0])
        for i in range(1, X):
            picked = jnp.where(c == i, values[i], picked)
        return picked

    def by_column(values, work):
        for value in sorted(set(values)):
            here = [x == c for c in range(X) if values[c] == value]
            pl.when(functools.reduce(jnp.logical_or, here))(functools.partial(work, value))

    def rows(k, size=None):
        return pl.ds(pl.multiple_of(k * R, R), R if size is None else size)

    def wait_for(ref, sem):
        pltpu.make_async_copy(ref, ref, sem).wait()

    def load_own(size):
        start = pl.multiple_of(of(begin, x), 16)
        return pltpu.make_async_copy(sig.at[pl.ds(start, size)], row.at[x, :size], load_sem.at[2])

    barrier = pltpu.get_barrier_semaphore()

    def meet(condition, peer):
        @pl.when(condition)
        def _():
            pl.semaphore_signal(barrier, inc=1, device_id=peer, device_id_type=MESH)

    for c in range(1, X):
        meet(c > x, at_x(c))
    meet(y < Y - 1, at_y(along_y(1)))
    meet(y == 0, at_y(along_y(Y - 1)))

    loads = []
    for part in range(2):
        for c in range(X):
            start, stop = ((0, LEAD * R), (LEAD * R, share[c]))[part]
            piece = pl.ds(begin[c] + start, stop - start)
            loads.append(pltpu.make_async_copy(sig.at[piece], mine.at[piece], load_sem.at[part]))
    load_gain = pltpu.make_async_copy(gain_in, gain, load_sem.at[3])
    for load in loads:
        load.start()
    by_column(share, lambda size: load_own(size).start())
    load_gain.start()
    acc[...] = jnp.zeros_like(acc)
    met = x + jnp.where(y > 0, 1, 0) + jnp.where(y == Y - 1, 1, 0)

    @pl.when(met > 0)
    def _():
        pl.semaphore_wait(barrier, met)

    for c in range(X - 1):

        @pl.when(c < x)
        def _(c=c):
            pl.semaphore_signal(ready.at[x], inc=1, device_id=at_x(c), device_id_type=MESH)

    @pl.when(y > 0)
    def _():
        pl.semaphore_signal(ready.at[0], inc=1, device_id=at_y(along_y(Y - 1)), device_id_type=MESH)

    def send_in(c, k, size=None):
        start = pl.multiple_of((of(begin, c) if size is None else begin[c]) + k * R, 16)
        pltpu.make_async_remote_copy(
            src_ref=mine.at[pl.ds(start, R if size is None else size)],
            dst_ref=row.at[x, rows(k, size)],
            send_sem=in_send,
            recv_sem=in_recv.at[k],
            device_id=at_x(c),
            device_id_type=MESH,
        ).start()

    def send_up(c, k, size=None):
        pltpu.make_async_remote_copy(
            src_ref=row.at[c, rows(k, size)],
            dst_ref=below.at[c - 1, rows(k, size)],
            send_sem=up_send,
            recv_sem=up_recv.at[k],
            device_id=at_y(along_y(1)),
            device_id_type=MESH,
        ).start()

    def send_out(d, k, size=None):
        c = along_x(d)
        pltpu.make_async_remote_copy(
            src_ref=mixed.at[c, rows(k, size)],
            dst_ref=back.at[x, rows(k, size)],
            send_sem=out_send,
            recv_sem=out_recv.at[k],
            device_id=at_x(c),
            device_id_type=MESH,
        ).start()

    def three(ref, k, size=None):
        return ref.at[: X - 1, rows(k, size)]

    for load in loads[:X]:
        load.wait()
    for d in (2, 3, 1):
        for c in range(X - 1):
            for k in range(LEAD):

                @pl.when(jnp.logical_and(c < x, along_x(d) == c))
                def _(c=c, k=k):
                    send_in(c, k)

    for c in range(1, X):

        @pl.when(c > x)
        def _(c=c):
            pl.semaphore_wait(ready.at[c], 1)
            for k in range(LEAD):
                send_in(c, k)

    for load in loads[X:]:
        load.wait()

    def to_others(k, whole):
        for c in (0, 2, 1, 3):

            @pl.when(x != c)
            def _(c=c):
                send_in(c, k, R if whole else tail[c])

    @pl.loop(LEAD, last)
    def _(k):
        to_others(k, True)

    to_others(last, False)
    by_column(share, lambda size: load_own(size).wait())

    @pl.when(y < Y - 1)
    def _():
        pl.semaphore_wait(ready.at[0], 1)

    @pl.when(x > 0)
    def _():
        @pl.loop(0, last)
        def _(k):
            send_up(x, k)

        by_column(tail, lambda size: send_up(x, last, size))

    load_gain.wait()

    def gather(k, size=None):
        wait_for(three(row, k, size), in_recv.at[k])
        for c in range(1, X):

            @pl.when(x != c)
            def _(c=c):
                send_up(c, k, size)

    def mix(k, size=None):
        size = R if size is None else size
        wait_for(three(below, k, size), up_recv.at[k])
        g0, g1, g2 = (jnp.broadcast_to(gain[i : i + 1, :], (8, gain.shape[1])) for i in range(3))

        def block(i, total):
            at = pl.ds(pl.multiple_of(k * R + i * BLOCK, BLOCK), BLOCK)
            taps = [below[c, at, :] for c in range(X - 1)] + [row[c, at, :] for c in range(X)]
            taps = [t.astype(jnp.float32).reshape(BLOCK // 8, 8, -1) for t in taps]
            for c in range(X):
                m = g0 * taps[c + 3] + g1 * taps[c + 1] + g2 * taps[c]
                total = total + jnp.sum(m * m, axis=0)
                mixed[c, at, :] = m.reshape(BLOCK, -1).astype(jnp.bfloat16)
            return total

        acc[...] = lax.fori_loop(0, size // BLOCK, block, acc[...])

    def give_back(k, size=None):
        for d in (2, 1, 3):
            send_out(d, k, size)

    gather(0)

    @pl.loop(1, EARLY + 1)
    def _(k):
        gather(k)
        mix(k - 1)
        give_back(k - 1)

    @pl.loop(EARLY + 1, last)
    def _(k):
        gather(k)
        mix(k - 1)

    by_column(tail, lambda size: gather(last, size))
    mix(last - 1)
    by_column(tail, lambda size: mix(last, size))

    for d in range(1, Y):
        pltpu.make_async_remote_copy(
            src_ref=acc, dst_ref=part_y.at[d - 1], send_sem=power_send.at[0], recv_sem=power_recv.at[0],
            device_id=at_y(along_y(d)), device_id_type=MESH,
        ).start()
    wait_for(part_y, power_recv.at[0])
    sum_y[...] = acc[...] + jnp.sum(part_y[...], axis=0)
    for d in range(1, X):
        pltpu.make_async_remote_copy(
            src_ref=sum_y, dst_ref=part_x.at[d - 1], send_sem=power_send.at[1], recv_sem=power_recv.at[1],
            device_id=at_x(along_x(d)), device_id_type=MESH,
        ).start()

    @pl.loop(EARLY, last)
    def _(k):
        give_back(k)

    by_column(tail, lambda size: give_back(last, size))

    wait_for(part_x, power_recv.at[1])
    total = sum_y[...] + jnp.sum(part_x[...], axis=0)
    power = jnp.sum(total, axis=0, keepdims=True) / (X * even * phases)
    scale = jnp.broadcast_to(lax.rsqrt(power + 1e-05), (8, out.shape[1]))

    def finish(source, c, begins, start, size):
        m = source[c, pl.ds(start, size), :].astype(jnp.float32).reshape(size // 8, 8, -1) * scale
        at = pl.ds(pl.multiple_of(begins + start, 16), size)
        out[at, :] = m.reshape(size, -1).astype(jnp.bfloat16)

    def finish_piece(source, c, k):
        begins = of(begin, c)

        @pl.loop(0, R // WIDE)
        def _(i):
            finish(source, c, begins, pl.multiple_of(k * R + i * WIDE, 16), WIDE)

    @pl.loop(0, last)
    def _(k):
        finish_piece(mixed, x, k)

    by_column(tail, lambda size: finish(mixed, x, of(begin, x), last * R, size))

    @pl.loop(0, last)
    def _(k):
        wait_for(three(back, k), out_recv.at[k])
        for d in range(1, X):
            finish_piece(back, along_x(d), k)

    by_column([sum(tail) - t for t in tail], lambda n: wait_for(mine.at[:n], out_recv.at[last]))
    for c in range(X):

        @pl.when(x != c)
        def _(c=c):
            finish(back, c, begin[c], last * R, tail[c])

    by_column([sum(share) - t for t in share], lambda n: wait_for(mine.at[:n], in_send))
    by_column(share, lambda size: wait_for(below.at[:, :size], up_send))
    by_column(share, lambda size: wait_for(below.at[:, :size], out_send))
    wait_for(part_y, power_send.at[0])
    wait_for(part_x, power_send.at[1])


def body(signal, tap_gain):
    steps, channels = signal.shape[2:]
    Y = lax.axis_size("phase") // X
    part = steps // X + max(SHIFT)
    pieces = whole_pieces(steps // X) + 1
    dma = pltpu.SemaphoreType.DMA

    def rows(n):
        return pltpu.VMEM((n, part, channels), jnp.bfloat16)

    def sums(*n):
        return pltpu.VMEM((*n, 8, channels), jnp.float32)

    out = pl.pallas_call(
        kernel,
        name="echoes",
        out_shape=pltpu.VMEM((steps, channels), signal.dtype),
        in_specs=[pl.BlockSpec(memory_space=pltpu.HBM)] * 2,
        out_specs=pl.BlockSpec(memory_space=pltpu.VMEM),
        scratch_shapes=[
            pltpu.VMEM(tap_gain.shape, jnp.float32),
            pltpu.VMEM((steps, channels), jnp.bfloat16),
            rows(X),
            rows(X - 1),
            rows(X),
            rows(X),
            sums(),
            sums(X - 1),
            sums(Y - 1),
            sums(),
            pltpu.SemaphoreType.REGULAR((X,)),
            dma((4,)),
            dma(()),
            dma((pieces,)),
            dma(()),
            dma((pieces,)),
            dma(()),
            dma((pieces,)),
            dma((2,)),
            dma((2,)),
        ],
        compiler_params=pltpu.CompilerParams(
            collective_id=0, has_side_effects=True, vmem_limit_bytes=VMEM
        ),
    )(signal.reshape(steps, channels), tap_gain)
    return out.reshape(signal.shape)


def solution(mesh):
    return jax.shard_map(
        body,
        mesh=mesh,
        in_specs=(P("phase", "line", None, None), P()),
        out_specs=P("phase", "line", None, None),
        check_vma=False,
    )
```

```python
import functools

import jax
import jax.numpy as jnp
from jax import lax
from jax.experimental import pallas as pl
from jax.experimental.pallas import tpu as pltpu
from jax.sharding import PartitionSpec as P

MESH = pl.DeviceIdType.MESH
X = 4
ROWS = 272
LAG = 1
SHIFT = (-32, 32, 48, -48)
EARLY = 6
LEAD = 1
BLOCK = 16
WIDE = 272
MIB = 2**20
VMEM = 54 * MIB


def whole_pieces(even):
    return (even + min(SHIFT) - 1) // ROWS


def kernel(
    sig, gain_in, out, gain, mine, row, below, mixed, back, acc, part_x, part_y, sum_y,
    ready, load_sem, in_send, in_recv, up_send, up_recv, out_send, out_recv, power_send, power_recv,
):
    me = lax.axis_index("phase")
    phases = lax.axis_size("phase")
    Y = phases // X
    x, y = lax.rem(me, X), me // X
    even = out.shape[0] // X
    R, last = ROWS, whole_pieces(even)
    share = [even + SHIFT[c] for c in range(X)]
    begin = [sum(share[:c]) for c in range(X)]
    tail = [share[c] - last * R for c in range(X)]

    def along_x(d):
        return lax.rem(x + d, X)

    def along_y(d):
        return lax.rem(y + d, Y)

    def at_x(c):
        return {"phase": y * X + c}

    def at_y(r):
        return {"phase": r * X + x}

    def of(values, c):
        picked = jnp.int32(values[0])
        for i in range(1, X):
            picked = jnp.where(c == i, values[i], picked)
        return picked

    def by_column(values, work):
        for value in sorted(set(values)):
            here = [x == c for c in range(X) if values[c] == value]
            pl.when(functools.reduce(jnp.logical_or, here))(functools.partial(work, value))

    def rows(k, size=None):
        return pl.ds(pl.multiple_of(k * R, R), R if size is None else size)

    def wait_for(ref, sem):
        pltpu.make_async_copy(ref, ref, sem).wait()

    def load_own(size):
        start = pl.multiple_of(of(begin, x), 16)
        return pltpu.make_async_copy(sig.at[pl.ds(start, size)], row.at[x, :size], load_sem.at[2])

    barrier = pltpu.get_barrier_semaphore()

    def meet(condition, peer):
        @pl.when(condition)
        def _():
            pl.semaphore_signal(barrier, inc=1, device_id=peer, device_id_type=MESH)

    for c in range(1, X):
        meet(c > x, at_x(c))
    meet(y < Y - 1, at_y(along_y(1)))
    meet(y == 0, at_y(along_y(Y - 1)))

    loads = []
    for part in range(2):
        for c in range(X):
            start, stop = ((0, LEAD * R), (LEAD * R, share[c]))[part]
            piece = pl.ds(begin[c] + start, stop - start)
            loads.append(pltpu.make_async_copy(sig.at[piece], mine.at[piece], load_sem.at[part]))
    load_gain = pltpu.make_async_copy(gain_in, gain, load_sem.at[3])
    for load in loads:
        load.start()
    by_column(share, lambda size: load_own(size).start())
    load_gain.start()
    acc[...] = jnp.zeros_like(acc)
    met = x + jnp.where(y > 0, 1, 0) + jnp.where(y == Y - 1, 1, 0)

    @pl.when(met > 0)
    def _():
        pl.semaphore_wait(barrier, met)

    for c in range(X - 1):

        @pl.when(c < x)
        def _(c=c):
            pl.semaphore_signal(ready.at[x], inc=1, device_id=at_x(c), device_id_type=MESH)

    @pl.when(y > 0)
    def _():
        pl.semaphore_signal(ready.at[0], inc=1, device_id=at_y(along_y(Y - 1)), device_id_type=MESH)

    def send_in(c, k, size=None):
        start = pl.multiple_of((of(begin, c) if size is None else begin[c]) + k * R, 16)
        pltpu.make_async_remote_copy(
            src_ref=mine.at[pl.ds(start, R if size is None else size)],
            dst_ref=row.at[x, rows(k, size)],
            send_sem=in_send,
            recv_sem=in_recv.at[k],
            device_id=at_x(c),
            device_id_type=MESH,
        ).start()

    def send_up(c, k, size=None):
        pltpu.make_async_remote_copy(
            src_ref=row.at[c, rows(k, size)],
            dst_ref=below.at[c - 1, rows(k, size)],
            send_sem=up_send,
            recv_sem=up_recv.at[k],
            device_id=at_y(along_y(1)),
            device_id_type=MESH,
        ).start()

    def send_out(d, k, size=None):
        c = along_x(d)
        pltpu.make_async_remote_copy(
            src_ref=mixed.at[c, rows(k, size)],
            dst_ref=back.at[x, rows(k, size)],
            send_sem=out_send,
            recv_sem=out_recv.at[k],
            device_id=at_x(c),
            device_id_type=MESH,
        ).start()

    def three(ref, k, size=None):
        return ref.at[: X - 1, rows(k, size)]

    for load in loads[:X]:
        load.wait()
    for c in range(X - 1):
        for k in range(LEAD):

            @pl.when(c < x)
            def _(c=c, k=k):
                send_in(c, k)

    for c in range(1, X):

        @pl.when(c > x)
        def _(c=c):
            pl.semaphore_wait(ready.at[c], 1)
            for k in range(LEAD):
                send_in(c, k)

    for load in loads[X:]:
        load.wait()

    def to_others(k, whole):
        for c in (0, 2, 1, 3):

            @pl.when(x != c)
            def _(c=c):
                send_in(c, k, R if whole else tail[c])

    @pl.loop(LEAD, last)
    def _(k):
        to_others(k, True)

    to_others(last, False)
    by_column(share, lambda size: load_own(size).wait())

    @pl.when(y < Y - 1)
    def _():
        pl.semaphore_wait(ready.at[0], 1)

    @pl.when(x > 0)
    def _():
        @pl.loop(0, last)
        def _(k):
            send_up(x, k)

        by_column(tail, lambda size: send_up(x, last, size))

    load_gain.wait()

    def gather(k, size=None):
        wait_for(three(row, k, size), in_recv.at[k])
        for c in range(1, X):

            @pl.when(x != c)
            def _(c=c):
                send_up(c, k, size)

    def mix(k, size=None):
        size = R if size is None else size
        wait_for(three(below, k, size), up_recv.at[k])
        g0, g1, g2 = (jnp.broadcast_to(gain[i : i + 1, :], (8, gain.shape[1])) for i in range(3))

        def block(i, total):
            at = pl.ds(pl.multiple_of(k * R + i * BLOCK, BLOCK), BLOCK)
            taps = [below[c, at, :] for c in range(X - 1)] + [row[c, at, :] for c in range(X)]
            taps = [t.astype(jnp.float32).reshape(BLOCK // 8, 8, -1) for t in taps]
            for c in range(X):
                m = g0 * taps[c + 3] + g1 * taps[c + 1] + g2 * taps[c]
                total = total + jnp.sum(m * m, axis=0)
                mixed[c, at, :] = m.reshape(BLOCK, -1).astype(jnp.bfloat16)
            return total

        acc[...] = lax.fori_loop(0, size // BLOCK, block, acc[...])

    def give_back(k, size=None):
        for d in (2, 1, 3):
            send_out(d, k, size)

    gather(0)

    @pl.loop(1, EARLY + 1)
    def _(k):
        gather(k)
        mix(k - 1)
        give_back(k - 1)

    @pl.loop(EARLY + 1, last)
    def _(k):
        gather(k)
        mix(k - 1)

    by_column(tail, lambda size: gather(last, size))
    mix(last - 1)
    by_column(tail, lambda size: mix(last, size))

    for d in range(1, Y):
        pltpu.make_async_remote_copy(
            src_ref=acc, dst_ref=part_y.at[d - 1], send_sem=power_send.at[0], recv_sem=power_recv.at[0],
            device_id=at_y(along_y(d)), device_id_type=MESH,
        ).start()
    wait_for(part_y, power_recv.at[0])
    sum_y[...] = acc[...] + jnp.sum(part_y[...], axis=0)
    for d in range(1, X):
        pltpu.make_async_remote_copy(
            src_ref=sum_y, dst_ref=part_x.at[d - 1], send_sem=power_send.at[1], recv_sem=power_recv.at[1],
            device_id=at_x(along_x(d)), device_id_type=MESH,
        ).start()

    @pl.loop(EARLY, last)
    def _(k):
        give_back(k)

    by_column(tail, lambda size: give_back(last, size))

    wait_for(part_x, power_recv.at[1])
    total = sum_y[...] + jnp.sum(part_x[...], axis=0)
    power = jnp.sum(total, axis=0, keepdims=True) / (X * even * phases)
    scale = jnp.broadcast_to(lax.rsqrt(power + 1e-05), (8, out.shape[1]))

    def finish(source, c, begins, start, size):
        m = source[c, pl.ds(start, size), :].astype(jnp.float32).reshape(size // 8, 8, -1) * scale
        at = pl.ds(pl.multiple_of(begins + start, 16), size)
        out[at, :] = m.reshape(size, -1).astype(jnp.bfloat16)

    def finish_piece(source, c, k):
        begins = of(begin, c)

        @pl.loop(0, R // WIDE)
        def _(i):
            finish(source, c, begins, pl.multiple_of(k * R + i * WIDE, 16), WIDE)

    @pl.loop(0, last)
    def _(k):
        finish_piece(mixed, x, k)

    by_column(tail, lambda size: finish(mixed, x, of(begin, x), last * R, size))

    @pl.loop(0, last)
    def _(k):
        wait_for(three(back, k), out_recv.at[k])
        for d in range(1, X):
            finish_piece(back, along_x(d), k)

    by_column([sum(tail) - t for t in tail], lambda n: wait_for(mine.at[:n], out_recv.at[last]))
    for c in range(X):

        @pl.when(x != c)
        def _(c=c):
            finish(back, c, begin[c], last * R, tail[c])

    by_column([sum(share) - t for t in share], lambda n: wait_for(mine.at[:n], in_send))
    by_column(share, lambda size: wait_for(below.at[:, :size], up_send))
    by_column(share, lambda size: wait_for(below.at[:, :size], out_send))
    wait_for(part_y, power_send.at[0])
    wait_for(part_x, power_send.at[1])


def body(signal, tap_gain):
    steps, channels = signal.shape[2:]
    Y = lax.axis_size("phase") // X
    part = steps // X + max(SHIFT)
    pieces = whole_pieces(steps // X) + 1
    dma = pltpu.SemaphoreType.DMA

    def rows(n):
        return pltpu.VMEM((n, part, channels), jnp.bfloat16)

    def sums(*n):
        return pltpu.VMEM((*n, 8, channels), jnp.float32)

    out = pl.pallas_call(
        kernel,
        name="echoes",
        out_shape=pltpu.VMEM((steps, channels), signal.dtype),
        in_specs=[pl.BlockSpec(memory_space=pltpu.HBM)] * 2,
        out_specs=pl.BlockSpec(memory_space=pltpu.VMEM),
        scratch_shapes=[
            pltpu.VMEM(tap_gain.shape, jnp.float32),
            pltpu.VMEM((steps, channels), jnp.bfloat16),
            rows(X),
            rows(X - 1),
            rows(X),
            rows(X),
            sums(),
            sums(X - 1),
            sums(Y - 1),
            sums(),
            pltpu.SemaphoreType.REGULAR((X,)),
            dma((4,)),
            dma(()),
            dma((pieces,)),
            dma(()),
            dma((pieces,)),
            dma(()),
            dma((pieces,)),
            dma((2,)),
            dma((2,)),
        ],
        compiler_params=pltpu.CompilerParams(
            collective_id=0, has_side_effects=True, vmem_limit_bytes=VMEM
        ),
    )(signal.reshape(steps, channels), tap_gain)
    return out.reshape(signal.shape)


def solution(mesh):
    return jax.shard_map(
        body,
        mesh=mesh,
        in_specs=(P("phase", "line", None, None), P()),
        out_specs=P("phase", "line", None, None),
        check_vma=False,
    )
```

```python
import functools

import jax
import jax.numpy as jnp
from jax import lax
from jax.experimental import pallas as pl
from jax.experimental.pallas import tpu as pltpu
from jax.sharding import PartitionSpec as P

MESH = pl.DeviceIdType.MESH
X = 4
ROWS = 272
LAG = 1
SHIFT = (-32, 32, 48, -48)
EARLY = 6
LEAD = 1
BLOCK = 16
WIDE = 272
MIB = 2**20
VMEM = 54 * MIB


def whole_pieces(even):
    return (even + min(SHIFT) - 1) // ROWS


def kernel(
    sig, gain_in, out, gain, mine, row, below, mixed, back, acc, part_x, part_y, sum_y,
    ready, load_sem, in_send, in_recv, up_send, up_recv, out_send, out_recv, power_send, power_recv,
):
    me = lax.axis_index("phase")
    phases = lax.axis_size("phase")
    Y = phases // X
    x, y = lax.rem(me, X), me // X
    even = out.shape[0] // X
    R, last = ROWS, whole_pieces(even)
    share = [even + SHIFT[c] for c in range(X)]
    begin = [sum(share[:c]) for c in range(X)]
    tail = [share[c] - last * R for c in range(X)]

    def along_x(d):
        return lax.rem(x + d, X)

    def along_y(d):
        return lax.rem(y + d, Y)

    def at_x(c):
        return {"phase": y * X + c}

    def at_y(r):
        return {"phase": r * X + x}

    def of(values, c):
        picked = jnp.int32(values[0])
        for i in range(1, X):
            picked = jnp.where(c == i, values[i], picked)
        return picked

    def by_column(values, work):
        for value in sorted(set(values)):
            here = [x == c for c in range(X) if values[c] == value]
            pl.when(functools.reduce(jnp.logical_or, here))(functools.partial(work, value))

    def rows(k, size=None):
        return pl.ds(pl.multiple_of(k * R, R), R if size is None else size)

    def wait_for(ref, sem):
        pltpu.make_async_copy(ref, ref, sem).wait()

    def load_own(size):
        start = pl.multiple_of(of(begin, x), 16)
        return pltpu.make_async_copy(sig.at[pl.ds(start, size)], row.at[x, :size], load_sem.at[2])

    barrier = pltpu.get_barrier_semaphore()

    def meet(condition, peer):
        @pl.when(condition)
        def _():
            pl.semaphore_signal(barrier, inc=1, device_id=peer, device_id_type=MESH)

    for c in range(1, X):
        meet(c > x, at_x(c))
    meet(y < Y - 1, at_y(along_y(1)))
    meet(y == 0, at_y(along_y(Y - 1)))

    loads = []
    for part in range(2):
        for c in range(X):
            start, stop = ((0, LEAD * R), (LEAD * R, share[c]))[part]
            piece = pl.ds(begin[c] + start, stop - start)
            loads.append(pltpu.make_async_copy(sig.at[piece], mine.at[piece], load_sem.at[part]))
    load_gain = pltpu.make_async_copy(gain_in, gain, load_sem.at[3])
    for load in loads:
        load.start()
    by_column(share, lambda size: load_own(size).start())
    load_gain.start()
    acc[...] = jnp.zeros_like(acc)
    met = x + jnp.where(y > 0, 1, 0) + jnp.where(y == Y - 1, 1, 0)

    @pl.when(met > 0)
    def _():
        pl.semaphore_wait(barrier, met)

    for c in range(X - 1):

        @pl.when(c < x)
        def _(c=c):
            pl.semaphore_signal(ready.at[x], inc=1, device_id=at_x(c), device_id_type=MESH)

    @pl.when(y > 0)
    def _():
        pl.semaphore_signal(ready.at[0], inc=1, device_id=at_y(along_y(Y - 1)), device_id_type=MESH)

    def send_in(c, k, size=None):
        start = pl.multiple_of((of(begin, c) if size is None else begin[c]) + k * R, 16)
        pltpu.make_async_remote_copy(
            src_ref=mine.at[pl.ds(start, R if size is None else size)],
            dst_ref=row.at[x, rows(k, size)],
            send_sem=in_send,
            recv_sem=in_recv.at[k],
            device_id=at_x(c),
            device_id_type=MESH,
        ).start()

    def send_up(c, k, size=None):
        pltpu.make_async_remote_copy(
            src_ref=row.at[c, rows(k, size)],
            dst_ref=below.at[c - 1, rows(k, size)],
            send_sem=up_send,
            recv_sem=up_recv.at[k],
            device_id=at_y(along_y(1)),
            device_id_type=MESH,
        ).start()

    def send_out(d, k, size=None):
        c = along_x(d)
        pltpu.make_async_remote_copy(
            src_ref=mixed.at[c, rows(k, size)],
            dst_ref=back.at[x, rows(k, size)],
            send_sem=out_send,
            recv_sem=out_recv.at[k],
            device_id=at_x(c),
            device_id_type=MESH,
        ).start()

    def three(ref, k, size=None):
        return ref.at[: X - 1, rows(k, size)]

    for load in loads[:X]:
        load.wait()
    for d in (2, 3, 1):
        for c in range(X - 1):
            for k in range(LEAD):

                @pl.when(jnp.logical_and(c < x, along_x(d) == c))
                def _(c=c, k=k):
                    send_in(c, k)

    for c in range(1, X):

        @pl.when(c > x)
        def _(c=c):
            pl.semaphore_wait(ready.at[c], 1)
            for k in range(LEAD):
                send_in(c, k)

    for load in loads[X:]:
        load.wait()

    def to_others(k, whole):
        for c in (0, 2, 1, 3):

            @pl.when(x != c)
            def _(c=c):
                send_in(c, k, R if whole else tail[c])

    @pl.loop(LEAD, last)
    def _(k):
        to_others(k, True)

    to_others(last, False)
    by_column(share, lambda size: load_own(size).wait())

    @pl.when(y < Y - 1)
    def _():
        pl.semaphore_wait(ready.at[0], 1)

    @pl.when(x > 0)
    def _():
        @pl.loop(0, last)
        def _(k):
            send_up(x, k)

        by_column(tail, lambda size: send_up(x, last, size))

    load_gain.wait()

    def gather(k, size=None):
        wait_for(three(row, k, size), in_recv.at[k])
        for c in range(1, X):

            @pl.when(x != c)
            def _(c=c):
                send_up(c, k, size)

    def mix(k, size=None):
        size = R if size is None else size
        wait_for(three(below, k, size), up_recv.at[k])
        g0, g1, g2 = (jnp.broadcast_to(gain[i : i + 1, :], (8, gain.shape[1])) for i in range(3))

        def block(i, total):
            at = pl.ds(pl.multiple_of(k * R + i * BLOCK, BLOCK), BLOCK)
            taps = [below[c, at, :] for c in range(X - 1)] + [row[c, at, :] for c in range(X)]
            taps = [t.astype(jnp.float32).reshape(BLOCK // 8, 8, -1) for t in taps]
            for c in range(X):
                m = g0 * taps[c + 3] + g1 * taps[c + 1] + g2 * taps[c]
                total = total + jnp.sum(m * m, axis=0)
                mixed[c, at, :] = m.reshape(BLOCK, -1).astype(jnp.bfloat16)
            return total

        acc[...] = lax.fori_loop(0, size // BLOCK, block, acc[...])

    def give_back(k, size=None):
        for d in (2, 1, 3):
            send_out(d, k, size)

    gather(0)

    @pl.loop(1, EARLY + 1)
    def _(k):
        gather(k)
        mix(k - 1)
        give_back(k - 1)

    @pl.loop(EARLY + 1, last)
    def _(k):
        gather(k)
        mix(k - 1)

    by_column(tail, lambda size: gather(last, size))
    mix(last - 1)
    by_column(tail, lambda size: mix(last, size))

    for d in range(1, Y):
        pltpu.make_async_remote_copy(
            src_ref=acc, dst_ref=part_y.at[d - 1], send_sem=power_send.at[0], recv_sem=power_recv.at[0],
            device_id=at_y(along_y(d)), device_id_type=MESH,
        ).start()
    wait_for(part_y, power_recv.at[0])
    sum_y[...] = acc[...] + jnp.sum(part_y[...], axis=0)
    for d in range(1, X):
        pltpu.make_async_remote_copy(
            src_ref=sum_y, dst_ref=part_x.at[d - 1], send_sem=power_send.at[1], recv_sem=power_recv.at[1],
            device_id=at_x(along_x(d)), device_id_type=MESH,
        ).start()

    @pl.loop(EARLY, last)
    def _(k):
        give_back(k)

    by_column(tail, lambda size: give_back(last, size))

    wait_for(part_x, power_recv.at[1])
    total = sum_y[...] + jnp.sum(part_x[...], axis=0)
    power = jnp.sum(total, axis=0, keepdims=True) / (X * even * phases)
    scale = jnp.broadcast_to(lax.rsqrt(power + 1e-05), (8, out.shape[1]))

    def finish(source, c, begins, start, size):
        m = source[c, pl.ds(start, size), :].astype(jnp.float32).reshape(size // 8, 8, -1) * scale
        at = pl.ds(pl.multiple_of(begins + start, 16), size)
        out[at, :] = m.reshape(size, -1).astype(jnp.bfloat16)

    def finish_piece(source, c, k):
        begins = of(begin, c)

        @pl.loop(0, R // WIDE)
        def _(i):
            finish(source, c, begins, pl.multiple_of(k * R + i * WIDE, 16), WIDE)

    @pl.loop(0, last)
    def _(k):
        finish_piece(mixed, x, k)

    by_column(tail, lambda size: finish(mixed, x, of(begin, x), last * R, size))

    @pl.loop(0, last)
    def _(k):
        wait_for(three(back, k), out_recv.at[k])
        for d in range(1, X):
            finish_piece(back, along_x(d), k)

    by_column([sum(tail) - t for t in tail], lambda n: wait_for(mine.at[:n], out_recv.at[last]))
    for c in range(X):

        @pl.when(x != c)
        def _(c=c):
            finish(back, c, begin[c], last * R, tail[c])

    by_column([sum(share) - t for t in share], lambda n: wait_for(mine.at[:n], in_send))
    by_column(share, lambda size: wait_for(below.at[:, :size], up_send))
    by_column(share, lambda size: wait_for(below.at[:, :size], out_send))
    wait_for(part_y, power_send.at[0])
    wait_for(part_x, power_send.at[1])


def body(signal, tap_gain):
    steps, channels = signal.shape[2:]
    Y = lax.axis_size("phase") // X
    part = steps // X + max(SHIFT)
    pieces = whole_pieces(steps // X) + 1
    dma = pltpu.SemaphoreType.DMA

    def rows(n):
        return pltpu.VMEM((n, part, channels), jnp.bfloat16)

    def sums(*n):
        return pltpu.VMEM((*n, 8, channels), jnp.float32)

    out = pl.pallas_call(
        kernel,
        name="echoes",
        out_shape=pltpu.VMEM((steps, channels), signal.dtype),
        in_specs=[pl.BlockSpec(memory_space=pltpu.HBM)] * 2,
        out_specs=pl.BlockSpec(memory_space=pltpu.VMEM),
        scratch_shapes=[
            pltpu.VMEM(tap_gain.shape, jnp.float32),
            pltpu.VMEM((steps, channels), jnp.bfloat16),
            rows(X),
            rows(X - 1),
            rows(X),
            rows(X),
            sums(),
            sums(X - 1),
            sums(Y - 1),
            sums(),
            pltpu.SemaphoreType.REGULAR((X,)),
            dma((4,)),
            dma(()),
            dma((pieces,)),
            dma(()),
            dma((pieces,)),
            dma(()),
            dma((pieces,)),
            dma((2,)),
            dma((2,)),
        ],
        compiler_params=pltpu.CompilerParams(
            collective_id=0, has_side_effects=True, vmem_limit_bytes=VMEM
        ),
    )(signal.reshape(steps, channels), tap_gain)
    return out.reshape(signal.shape)


def solution(mesh):
    return jax.shard_map(
        body,
        mesh=mesh,
        in_specs=(P("phase", "line", None, None), P()),
        out_specs=P("phase", "line", None, None),
        check_vma=False,
    )
```
